16 devices in a mesh: col: 4 (over z, y), row: 4 (over x, core).
Axes of the slice: x: 2, y: 2, z: 2, core: 2. Of those that a mesh axis runs over, the one named last changes fastest.
Arguments:
- t_amps: float32 [256, 20736], P('row', 'col')
- denoms: float32 [256, 20736], P('row', 'col')
- v_oovv: bfloat16 [256, 20736], P('row', 'col')
- v_vvvv: bfloat16 [20736, 20736], P('row', 'col')
- v_oooo: bfloat16 [256, 256], replicated
- w_direct: bfloat16 [2304, 2304], P(None, 'col')
- w_exch: bfloat16 [2304, 2304], P(None, 'col')
Outputs:
- output: float32 [256, 20736], P('row', 'col')
All inputs are finite; a program needn't handle non-finite values.
Results may differ from the reference program's by a relative error of at most 0.001.
Values are sent between devices in bfloat16 or wider.
A program may use at most 1 GiB of HBM per device.

```python
import jax
import jax.numpy as jnp

OCC = 16
VIRT = 144
PAIRS_OCC = OCC * OCC
PAIRS_VIRT = VIRT * VIRT
PH_DIM = OCC * VIRT


def setup_inputs(seed: int = 0) -> dict:
    keys = jax.random.split(jax.random.key(seed), 7)
    amp_scale = 1.5 * (OCC * VIRT) ** -0.5
    t_amps = amp_scale * jax.random.normal(keys[0], (PAIRS_OCC, PAIRS_VIRT), jnp.float32)
    denoms = -jax.random.uniform(keys[1], (PAIRS_OCC, PAIRS_VIRT), jnp.float32, 1.0, 3.0)
    v_oovv = jax.random.normal(keys[2], (PAIRS_OCC, PAIRS_VIRT), jnp.float32).astype(jnp.bfloat16)
    vvvv_scale = (OCC / VIRT) ** 0.5 / 1.5
    v_vvvv = (vvvv_scale * jax.random.normal(keys[3], (PAIRS_VIRT, PAIRS_VIRT), jnp.float32)).astype(jnp.bfloat16)
    oooo_scale = (VIRT / OCC) ** 0.5 / 1.5
    v_oooo = (oooo_scale * jax.random.normal(keys[4], (PAIRS_OCC, PAIRS_OCC), jnp.float32)).astype(jnp.bfloat16)
    w_direct = (0.6 * jax.random.normal(keys[5], (PH_DIM, PH_DIM), jnp.float32)).astype(jnp.bfloat16)
    w_exch = (0.6 * jax.random.normal(keys[6], (PH_DIM, PH_DIM), jnp.float32)).astype(jnp.bfloat16)
    return {"t_amps": t_amps, "denoms": denoms, "v_oovv": v_oovv, "v_vvvv": v_vvvv, "v_oooo": v_oooo, "w_direct": w_direct, "w_exch": w_exch}


def reference(t_amps, denoms, v_oovv, v_vvvv, v_oooo, w_direct, w_exch):
    t_half = t_amps.astype(jnp.bfloat16)
    ladder = jnp.dot(t_half, v_vvvv, preferred_element_type=jnp.float32)
    inter_x = jnp.dot(v_oovv, t_half.T, preferred_element_type=jnp.float32)
    hole_mat = (v_oooo.astype(jnp.float32) + 0.5 * inter_x).astype(jnp.bfloat16)
    hole_term = jnp.dot(hole_mat.T, t_half, preferred_element_type=jnp.float32)
    t_wide = t_half.astype(jnp.float32).reshape(OCC, OCC, VIRT, VIRT)
    wd_wide = w_direct.astype(jnp.float32).reshape(OCC, VIRT, OCC, VIRT)
    wx_wide = w_exch.astype(jnp.float32).reshape(OCC, VIRT, OCC, VIRT)
    direct_term = jnp.einsum("ikac,kcjb->ijab", t_wide, wd_wide)
    exch_term = jnp.einsum("ikcb,kcja->ijab", t_wide, wx_wide)
    ph_net = direct_term - exch_term
    ph_sym = (ph_net + ph_net.transpose(1, 0, 3, 2)).reshape(PAIRS_OCC, PAIRS_VIRT)
    residual = v_oovv.astype(jnp.float32) + ladder + hole_term + ph_sym
    return residual / denoms
```

```python
import functools
import math

import jax
import jax.numpy as jnp
from jax import lax
from jax.experimental import pallas as pl
from jax.experimental.pallas import tpu as pltpu
from jax.sharding import PartitionSpec as P

F32 = jnp.float32
BF16 = jnp.bfloat16
MESH = pl.DeviceIdType.MESH
CHUNK = 512
LANES = 128
NQ = 4


def sweep_kernel(
    dims,
    t_hbm, den_hbm, oovv_hbm, vvvv_hbm, vlast_hbm, oooo_hbm, wd_hbm, wx_hbm, perm_hbm, swap_hbm,
    out_hbm,
    t32, rows, lad, tcols, wd, wx, wxt, tr, r3, r5, sd, sp, msg_d, msg_p, got_d, got_p,
    part, half, xsend, xgot, vbuf, vlast, oovv, oooo, perm, swap, xpart, xgot_part, m_mine, m_got,
    in_sem, vb_sem, loc_sem, ts_sem, tr_sem, ls_sem, lr_sem, g_sem,
    ps_sem, pr_sem, d_sem, hs_sem, hr_sem, xs_sem, xr_sem, x_sem, m_sem,
):
    n_occ, n_virt, n_row, n_col = dims
    rows_dev, cols_dev = t32.shape
    occ = n_occ // n_row
    vir = n_virt // n_col
    qrows = rows_dev // NQ
    n_full = cols_dev // CHUNK
    tail = cols_dev - n_full * CHUNK
    r = lax.axis_index("row")
    c = lax.axis_index("col")
    x, u = r // 2, r % 2
    z, y = c // 2, c % 2
    c_y, c_z, c_d = 2 * z + 1 - y, 2 * (1 - z) + y, 2 * (1 - z) + 1 - y
    r_p, r_s, r_o = 2 * x + 1 - u, 2 * (1 - x) + u, 2 * (1 - x) + 1 - u
    col_peers = (c_y, c_z, c_d)
    row_peers = (r_p, r_s, r_o)

    def remote(src, dst, ssem, rsem, row, col):
        return pltpu.make_async_remote_copy(
            src_ref=src, dst_ref=dst, send_sem=ssem, recv_sem=rsem,
            device_id={"row": row, "col": col}, device_id_type=MESH)

    def load(src, dst, k):
        return pltpu.make_async_copy(src, dst, in_sem.at[k])

    ld_t = load(t_hbm, t32, 0)
    ld_wx = load(wx_hbm, wx, 1)
    ld_wd = load(wd_hbm, wd, 2)
    ld_oovv = load(oovv_hbm, oovv, 3)
    ld_oooo = load(oooo_hbm, oooo, 4)
    ld_perm = load(perm_hbm, perm, 5)
    ld_swap = load(swap_hbm, swap, 6)
    ld_den = load(den_hbm, t32, 7)
    for ld in (ld_t, ld_wx, ld_wd, ld_oovv, ld_oooo, ld_perm, ld_swap):
        ld.start()

    def fetch(off, width, slot):
        return pltpu.make_async_copy(vvvv_hbm.at[:, pl.ds(off, width)], vbuf.at[slot], vb_sem.at[slot])

    for s in range(2):
        fetch(s * CHUNK, CHUNK, s).start()
    ld_last = load(vlast_hbm, vlast, 9)
    ld_last.start()

    barrier = pltpu.get_barrier_semaphore()
    for p in col_peers:
        pl.semaphore_signal(barrier, inc=1, device_id={"row": r, "col": p}, device_id_type=MESH)
    for p in row_peers:
        pl.semaphore_signal(barrier, inc=1, device_id={"row": p, "col": c}, device_id_type=MESH)
    pl.semaphore_wait(barrier, 6)

    def piece(ref, k, q):
        return ref.at[k, pl.ds(q * qrows, qrows), :]

    def send_y(q):
        return remote(piece(rows, c, q), piece(rows, c, q), ts_sem.at[0, q], tr_sem.at[0, q], r, c_y)

    def send_z(q):
        return remote(piece(rows, c, q), piece(rows, c, q), ts_sem.at[1, q], tr_sem.at[1, q], r, c_z)

    def send_d(q):
        return remote(piece(rows, c_y, q), piece(rows, c_y, q), ts_sem.at[2, q], tr_sem.at[2, q], r, c_z)

    blk_x = 2 * (1 - x) + y

    def send_lx(q):
        return remote(piece(rows, blk_x, q), piece(lad, r, q), ls_sem.at[0, q], lr_sem.at[u, q], blk_x, c)

    def recv_lx(w, q):
        k = 2 * (1 - x) + w
        return remote(piece(lad, k, q), piece(lad, k, q), ls_sem.at[0, q], lr_sem.at[w, q], blk_x, c)

    def send_ly(w, q):
        k = 2 * (1 - x) + w
        return remote(piece(lad, k, q), piece(lad, k, q), ls_sem.at[1 + w, q], lr_sem.at[2 + w, q], r, c_y)

    own_ladder = z == 1 - x
    direct = u == y

    ld_t.wait()
    for q in range(NQ):
        rows[c, pl.ds(q * qrows, qrows), :] = t32[pl.ds(q * qrows, qrows), :].astype(BF16)
        send_y(q).start()
        send_z(q).start()

        @pl.when(own_ladder)
        def _():
            send_lx(q).start()

    ld_den.start()

    def row_send(k, p):
        return remote(rows.at[c], tcols.at[r], g_sem.at[0, k], g_sem.at[1, k], p, c)

    for k, p in enumerate(row_peers):
        row_send(k, p).start()

    tcols[r] = rows[c]

    ld_wx.wait()

    @pl.loop(0, wx.shape[0] // 128)
    def _(m):
        src = pl.ds(pl.multiple_of(m * 128, 128), 128)
        for b in range(0, wx.shape[1], 128):
            w = min(128, wx.shape[1] - b)
            wxt[b:b + w, src] = wx[src, b:b + w].astype(F32).T.astype(BF16)

    def forward_ladder(q):
        @pl.when(direct)
        def _():
            for w in range(2):
                recv_lx(w, q).wait_recv()
                send_ly(w, q).start()

    for q in range(NQ):
        send_z(q).wait_recv()

        @pl.when(jnp.logical_not(own_ladder))
        def _():
            send_lx(q).start()

        send_y(q).wait_recv()
        send_d(q).start()
        if q:
            forward_ladder(q - 1)
    forward_ladder(NQ - 1)
    for q in range(NQ):
        send_d(q).wait_recv()

    lad_p = remote(rows.at[r_p], lad.at[r], g_sem.at[0, 3], g_sem.at[1, 3], r_p, c)
    lad_p.start()
    lad[r] = rows[r]

    for k, p in enumerate(row_peers):
        row_send(k, p).wait_recv()
    ld_oovv.wait()
    for k in range(n_row):
        xpart[:, k * rows_dev:(k + 1) * rows_dev] = lax.dot_general(
            oovv[...], tcols[k], (((1,), (1,)), ((), ())), preferred_element_type=F32)

    def x_send(k, p):
        return remote(xpart, xgot_part.at[c], x_sem.at[0, k], x_sem.at[1, k], r, p)

    for k, p in enumerate(col_peers):
        x_send(k, p).start()

    ld_swap.wait()
    ld_wd.wait()

    @pl.loop(0, occ)
    def _(i):
        lines = pl.ds(pl.multiple_of(i * n_occ, n_occ), n_occ)
        for ab in range(n_virt // n_occ):
            stack = []
            for t in range(n_occ):
                a = ab * n_occ + t
                lo = (a % vir) * n_virt
                stack.append(rows[a // vir, lines, lo:lo + n_virt])
            turned = jnp.dot(swap[...], jnp.concatenate(stack, axis=0), preferred_element_type=F32).astype(BF16)
            for k in range(n_occ):
                tr[i, k * n_virt + ab * n_occ:k * n_virt + (ab + 1) * n_occ, :] = turned[k * n_occ:(k + 1) * n_occ]

        r5[...] = jnp.dot(wxt[...], tr[i], preferred_element_type=F32)
        r3[...] = jnp.dot(tr[i, 0:n_virt, :], wd[0:n_virt, :], preferred_element_type=F32)

        @pl.loop(1, n_occ)
        def _(k):
            at = pl.ds(pl.multiple_of(k * n_virt, 16), n_virt)
            r3[...] += jnp.dot(tr[i, at, :], wd[at, :], preferred_element_type=F32)

        for j in range(occ):
            diff = r3[:, j * n_virt:(j + 1) * n_virt] - r5[j * n_virt:(j + 1) * n_virt, :]
            sd[i * occ + j] = diff
            sp[j * occ + i] = diff.T

    n_pair = occ * occ
    pad = pl.ds(cols_dev - tail, LANES)
    for k in range(n_col):
        msg_p[k, :, pad] = jnp.zeros((n_pair, LANES), F32)
        msg_d[k, :, pad] = jnp.zeros((n_pair, LANES), F32)
        part[k, :, pad] = jnp.zeros((rows_dev, LANES), F32)

    @pl.loop(0, n_col)
    def _(k):
        for a in range(vir):
            msg_p[k, :, a * n_virt:(a + 1) * n_virt] = sp[:, k * vir + a, :]

    def p_send(off, width, n, k, p):
        at = pl.ds(off, width)
        return remote(msg_p.at[p, :, at], got_p.at[c, :, at], ps_sem.at[k, n], pr_sem.at[k, n], r, p)

    chunks = [(n * CHUNK, CHUNK) for n in range(n_full)] + [(n_full * CHUNK, LANES)]
    for n, (off, width) in enumerate(chunks):
        for k, p in enumerate(col_peers):
            p_send(off, width, n, k, p).start()
    own_p = pltpu.make_async_copy(msg_p.at[c], got_p.at[c], loc_sem.at[0])
    own_p.start()

    @pl.loop(0, n_col)
    def _(k):
        for a in range(vir):
            msg_d[k, :, a * n_virt:(a + 1) * n_virt] = sd[:, k * vir + a, :]

    def d_send(k, p):
        return remote(msg_d.at[p], got_d.at[c], d_sem.at[0, k], d_sem.at[1, k], r, p)

    for k, p in enumerate(col_peers):
        d_send(k, p).start()
    own_d = pltpu.make_async_copy(msg_d.at[c], got_d.at[c], loc_sem.at[1])
    own_d.start()

    for k, p in enumerate(col_peers):
        x_send(k, p).wait_recv()
    xgot_part[c] = xpart[...]
    x_sum = xgot_part[0] + xgot_part[1] + xgot_part[2] + xgot_part[3]
    ld_oooo.wait()
    hole = (oooo[pl.ds(pl.multiple_of(r * rows_dev, rows_dev), rows_dev), :].astype(F32) + 0.5 * x_sum)
    for k in range(n_row):
        m_mine[k] = hole[:, k * rows_dev:(k + 1) * rows_dev].astype(BF16)

    def m_send(k, p):
        return remote(m_mine.at[p], m_got.at[r], m_sem.at[0, k], m_sem.at[1, k], p, c)

    for k, p in enumerate(row_peers):
        m_send(k, p).start()
    m_got[r] = m_mine[r]

    lad_p.wait_recv()

    @pl.when(jnp.logical_not(direct))
    def _():
        for q in range(NQ):
            for w in range(2):
                send_ly(w, q).wait_recv()

    @pl.when(direct)
    def _():
        for q in range(NQ):
            for w in range(2):
                send_ly(w, q).wait_send()
    lad_p.wait_send()
    ld_perm.wait()

    @pl.loop(0, n_row)
    def _(k):
        for off in range(0, cols_dev, CHUNK):
            width = min(CHUNK, cols_dev - off)
            block = jnp.dot(perm[...], lad[k, :, off:off + width], preferred_element_type=F32)
            lad[k, :, off:off + width] = block.astype(BF16)

    own_p.wait()

    def h_send(off, width, n, w):
        at = pl.ds(off, width)
        return remote(part.at[2 * w + 1 - u, :, at], half.at[w, :, at], hs_sem.at[w, n], hr_sem.at[w, n], r_p, c)

    def x_pass(off, width, n):
        at = pl.ds(off, width)
        return remote(xsend.at[:, at], xgot.at[:, at], xs_sem.at[n], xr_sem.at[n], r_s, c)

    def across(off, width, n):
        at = pl.ds(off, width)
        for w in range(2):
            h_send(off, width, n, w).wait_recv()
        xsend[:, at] = part[2 * (1 - x) + u, :, at] + half[1 - x, :, at]
        x_pass(off, width, n).start()

    def ladder(off, width, n, v_ref):
        at = pl.ds(off, width)
        t_all = lad[...].reshape(n_row * rows_dev, cols_dev)
        prod = jnp.dot(t_all, v_ref[...], preferred_element_type=F32)
        part[:, :, pl.ds(off, prod.shape[1])] = prod.reshape(n_row, rows_dev, prod.shape[1])
        for k, p in enumerate(col_peers):
            p_send(off, width, n, k, p).wait_recv()
        mine = pl.ds(pl.multiple_of(r * n_pair, n_pair), n_pair)
        for k in range(n_col):
            part[k, mine, at] += got_p[k, :, at]
        for w in range(2):
            h_send(off, width, n, w).start()

    @pl.loop(0, n_full)
    def _(n):
        off = pl.multiple_of(n * CHUNK, CHUNK)
        fetch(off, CHUNK, n % 2).wait()
        ladder(off, CHUNK, n, vbuf.at[n % 2])

        @pl.when(n + 2 < n_full)
        def _():
            fetch(pl.multiple_of((n + 2) * CHUNK, CHUNK), CHUNK, n % 2).start()

        @pl.when(n >= 1)
        def _():
            across(pl.multiple_of((n - 1) * CHUNK, CHUNK), CHUNK, n - 1)

    ld_last.wait()
    ladder(n_full * CHUNK, LANES, n_full, vlast)
    across((n_full - 1) * CHUNK, CHUNK, n_full - 1)
    across(n_full * CHUNK, LANES, n_full)

    for k, p in enumerate(row_peers):
        m_send(k, p).wait_recv()
    for k, p in enumerate(col_peers):
        d_send(k, p).wait_recv()
    own_d.wait()
    ld_den.wait()

    def finish(off, width, n):
        at = pl.ds(off, width)
        hole_term = None
        for k in range(n_row):
            term = lax.dot_general(
                m_got[k], tcols[k, :, at], (((0,), (0,)), ((), ())), preferred_element_type=F32)
            hole_term = term if hole_term is None else hole_term + term
        own = part[r, :, at] + half[x, :, at] + xgot[:, at]
        for jh in range(n_col):
            v = own[jh * n_pair:(jh + 1) * n_pair] + got_d[jh, :, at]
            for i in range(occ):
                lo = i * n_occ + jh * occ
                xgot[lo:lo + occ, at] = v[i * occ:(i + 1) * occ]
        total = oovv[:, at].astype(F32) + xgot[:, at] + hole_term
        t32[:, at] = total / t32[:, at]

    @pl.loop(0, n_full)
    def _(n):
        off = pl.multiple_of(n * CHUNK, CHUNK)
        x_pass(off, CHUNK, n).wait_recv()
        finish(off, CHUNK, n)

    x_pass(n_full * CHUNK, LANES, n_full).wait_recv()
    finish(n_full * CHUNK, tail, n_full)
    st = pltpu.make_async_copy(t32, out_hbm, in_sem.at[8])
    st.start()

    for q in range(NQ):
        send_y(q).wait_send()
        send_z(q).wait_send()
        send_d(q).wait_send()
        send_lx(q).wait_send()
    for k, p in enumerate(row_peers):
        row_send(k, p).wait_send()
        m_send(k, p).wait_send()
    for k, p in enumerate(col_peers):
        x_send(k, p).wait_send()
        d_send(k, p).wait_send()
    for n, (off, width) in enumerate(chunks):
        for k, p in enumerate(col_peers):
            p_send(off, width, n, k, p).wait_send()
        for w in range(2):
            h_send(off, width, n, w).wait_send()
        x_pass(off, width, n).wait_send()
    st.wait()


def solution(mesh):
    n_row = mesh.shape["row"]
    n_col = mesh.shape["col"]
    amp_spec = P("row", "col")
    wide_spec = P(None, "col")

    def local_sweep(t_blk, d_blk, oovv_blk, vvvv_blk, oooo_full, wd_blk, wx_blk):
        rows_dev, cols_dev = t_blk.shape
        n_occ = math.isqrt(oooo_full.shape[0])
        n_virt = wd_blk.shape[0] // n_occ
        occ, vir = n_occ // n_row, n_virt // n_col
        n_pair = occ * occ
        n_chunk = cols_dev // CHUNK + 1
        v_last = vvvv_blk[:, cols_dev // CHUNK * CHUNK:]
        wide = -(-cols_dev // LANES) * LANES
        kc, jb = wd_blk.shape
        perm = jnp.eye(rows_dev, dtype=BF16).reshape(occ, n_col, occ, rows_dev).transpose(1, 0, 2, 3).reshape(rows_dev, rows_dev)
        n_sq = n_occ * n_occ
        swap = jnp.eye(n_sq, dtype=BF16).reshape(n_occ, n_occ, n_sq).transpose(1, 0, 2).reshape(n_sq, n_sq)
        dma = pltpu.SemaphoreType.DMA
        vm = pltpu.VMEM
        hbm = pl.BlockSpec(memory_space=pl.ANY)
        block = (rows_dev, cols_dev)
        return pl.pallas_call(
            functools.partial(sweep_kernel, (n_occ, n_virt, n_row, n_col)),
            out_shape=jax.ShapeDtypeStruct(block, F32),
            in_specs=[hbm] * 10,
            out_specs=hbm,
            scratch_shapes=[
                vm(block, F32), vm((n_col,) + block, BF16), vm((n_row,) + block, BF16), vm((n_row,) + block, BF16),
                vm((kc, jb), BF16), vm((kc, jb), BF16), vm((jb, kc), BF16),
                vm((occ, kc, n_virt), BF16), vm((n_virt, jb), F32), vm((jb, n_virt), F32),
                vm((n_pair, n_virt, n_virt), F32), vm((n_pair, n_virt, n_virt), F32),
                vm((n_col, n_pair, wide), F32), vm((n_col, n_pair, wide), F32),
                vm((n_col, n_pair, wide), F32), vm((n_col, n_pair, wide), F32),
                vm((n_row, rows_dev, wide), F32), vm((2, rows_dev, wide), F32),
                vm((rows_dev, wide), F32), vm((rows_dev, wide), F32),
                vm((2, cols_dev, CHUNK), BF16), vm(v_last.shape, BF16), vm(block, BF16), vm(oooo_full.shape, BF16),
                vm((rows_dev, rows_dev), BF16), vm((n_sq, n_sq), BF16),
                vm((rows_dev, n_sq), F32), vm((n_col, rows_dev, n_sq), F32),
                vm((n_row, rows_dev, rows_dev), BF16), vm((n_row, rows_dev, rows_dev), BF16),
                dma((10,)), dma((2,)), dma((2,)), dma((3, NQ)), dma((3, NQ)), dma((3, NQ)), dma((4, NQ)), dma((2, 4)),
                dma((3, n_chunk)), dma((3, n_chunk)), dma((2, 3)), dma((2, n_chunk)), dma((2, n_chunk)),
                dma((n_chunk,)), dma((n_chunk,)), dma((2, 3)), dma((2, 3)),
            ],
            compiler_params=pltpu.CompilerParams(
                collective_id=0, has_side_effects=True, vmem_limit_bytes=67043328),
        )(t_blk, d_blk, oovv_blk, vvvv_blk, v_last, oooo_full, wd_blk, wx_blk, perm, swap)

    return jax.shard_map(
        local_sweep, mesh=mesh,
        in_specs=(amp_spec, amp_spec, amp_spec, amp_spec, P(), wide_spec, wide_spec),
        out_specs=amp_spec, check_vma=False)
```

```python
import functools
import math

import jax
import jax.numpy as jnp
import numpy as np
from jax import lax
from jax.experimental import pallas as pl
from jax.experimental.pallas import tpu as pltpu
from jax.sharding import PartitionSpec as P

F32 = jnp.float32
BF16 = jnp.bfloat16
MESH = pl.DeviceIdType.MESH
CHUNK = 512
LANES = 128
P_AHEAD = 3
AHEAD = 2
OVER_Y = 1
FORWARD = ((2, (0,)), (3, (1,)), (4, (2, 3)))
NQ = 4


def sweep_kernel(
    dims,
    t_hbm, den_hbm, oovv_hbm, vvvv_hbm, vlast, oooo_hbm, wd_hbm, wx_hbm, perm_hbm, swap_hbm,
    out_hbm,
    t32, rows, lad, tcols, wd, wdt, wxt, tr, ta, r3, r5, sd, sp, msg_d, msg_p, got_d, got_p,
    part, half, xsend, xgot, vbuf, oovv, oooo, perm, swap, xpart, xgot_part, m_mine, m_got,
    in_sem, vb_sem, loc_sem, ts_sem, tr_sem, ls_sem, lr_sem, g_sem,
    rx_sem, ps_sem, pr_sem, d_sem, hs_sem, hr_sem, xs_sem, xr_sem, x_sem, m_sem,
):
    n_occ, n_virt, n_row, n_col = dims
    rows_dev, cols_dev = t32.shape
    occ = n_occ // n_row
    vir = n_virt // n_col
    qrows = rows_dev // NQ
    n_full = cols_dev // CHUNK
    tail = cols_dev - n_full * CHUNK
    r = lax.axis_index("row")
    c = lax.axis_index("col")
    x, u = r // 2, r % 2
    z, y = c // 2, c % 2
    c_y, c_z, c_d = 2 * z + 1 - y, 2 * (1 - z) + y, 2 * (1 - z) + 1 - y
    r_p, r_s, r_o = 2 * x + 1 - u, 2 * (1 - x) + u, 2 * (1 - x) + 1 - u
    col_peers = (c_y, c_z, c_d)
    row_peers = (r_p, r_s, r_o)

    def remote(src, dst, ssem, rsem, row, col):
        return pltpu.make_async_remote_copy(
            src_ref=src, dst_ref=dst, send_sem=ssem, recv_sem=rsem,
            device_id={"row": row, "col": col}, device_id_type=MESH)

    def load(src, dst, k):
        return pltpu.make_async_copy(src, dst, in_sem.at[k])

    ld_t = load(t_hbm, t32, 0)
    ld_wx = load(wx_hbm, wxt, 1)
    ld_wd = load(wd_hbm, wdt, 2)
    ld_oovv = load(oovv_hbm, oovv, 3)
    ld_oooo = load(oooo_hbm, oooo, 4)
    ld_perm = load(perm_hbm, perm, 5)
    ld_swap = load(swap_hbm, swap, 6)
    ld_den = load(den_hbm, t32, 7)
    for ld in (ld_t, ld_wx, ld_wd, ld_oovv, ld_oooo, ld_perm, ld_swap):
        ld.start()

    def fetch(off, width, slot):
        return pltpu.make_async_copy(vvvv_hbm.at[:, pl.ds(off, width)], vbuf.at[slot], vb_sem.at[slot])

    for s in range(2):
        fetch(s * CHUNK, CHUNK, s).start()

    barrier = pltpu.get_barrier_semaphore()
    for p in col_peers:
        pl.semaphore_signal(barrier, inc=1, device_id={"row": r, "col": p}, device_id_type=MESH)
    for p in row_peers:
        pl.semaphore_signal(barrier, inc=1, device_id={"row": p, "col": c}, device_id_type=MESH)
    pl.semaphore_wait(barrier, 6)

    def piece(ref, k, q):
        return ref.at[k, pl.ds(pl.multiple_of(q * qrows, qrows), qrows), :]

    def send_y(q):
        return remote(piece(rows, c, q), piece(rows, c, q), ts_sem.at[0, q], tr_sem.at[0, q], r, c_y)

    def send_z(q):
        return remote(piece(rows, c, q), piece(rows, c, q), ts_sem.at[1, q], tr_sem.at[1, q], r, c_z)

    def send_dz(q):
        return remote(piece(rows, c_y, q), piece(rows, c_y, q), ts_sem.at[2, q], tr_sem.at[2, q], r, c_z)

    def send_dy(q):
        return remote(piece(rows, c_z, q), piece(rows, c_z, q), ts_sem.at[2, q], tr_sem.at[2, q], r, c_y)

    blk_x = 2 * (1 - x) + y

    def send_lx(q):
        return remote(piece(rows, blk_x, q), piece(lad, r, q), ls_sem.at[0, q], lr_sem.at[u, q], blk_x, c)

    def recv_lx(w, q):
        k = 2 * (1 - x) + w
        return remote(piece(lad, k, q), piece(lad, k, q), ls_sem.at[0, q], lr_sem.at[w, q], blk_x, c)

    def send_ly(w, q):
        k = 2 * (1 - x) + w
        return remote(piece(lad, k, q), piece(lad, k, q), ls_sem.at[1 + w, q], lr_sem.at[2 + w, q], r, c_y)

    own_ladder = z == 1 - x
    direct = u == y

    ld_t.wait()
    for q in range(NQ):
        rows[c, pl.ds(q * qrows, qrows), :] = t32[pl.ds(q * qrows, qrows), :].astype(BF16)
        if q < AHEAD:
            send_y(q).start()
            send_z(q).start()

            @pl.when(own_ladder)
            def _():
                send_lx(q).start()

    ld_den.start()

    def send_row(q):
        return remote(piece(rows, c, q), piece(tcols, r, q), rx_sem.at[0, q], rx_sem.at[1, q], r_s, c)

    row_p = remote(rows.at[c], tcols.at[r], g_sem.at[0, 0], g_sem.at[1, 0], r_p, c)
    row_o = remote(tcols.at[r_s], tcols.at[r_s], g_sem.at[0, 1], g_sem.at[1, 1], r_p, c)
    row_p.start()
    send_row(0).start()
    tcols[r] = rows[c]

    with jax.named_scope("ph_turn_w"):
        ld_wd.wait()

        @pl.loop(0, wd.shape[0] // LANES)
        def _(m):
            at = pl.ds(pl.multiple_of(m * LANES, LANES), LANES)
            for b in range(0, wd.shape[1], LANES):
                w = min(LANES, wd.shape[1] - b)
                wd[at, b:b + w] = wdt[b:b + w, at].astype(F32).T.astype(BF16)

    def forward_ladder(q):
        @pl.when(direct)
        def _():
            for w in range(2):
                recv_lx(w, q).wait_recv()
                send_ly(w, q).start()

    ld_swap.wait()
    ld_wx.wait()

    def spread(i):
        lines = pl.ds(pl.multiple_of(i * n_occ, n_occ), n_occ)
        for ab in range(n_virt // n_occ):
            stack = []
            for t in range(n_occ):
                a = ab * n_occ + t
                lo = (a % vir) * n_virt
                stack.append(rows[a // vir, lines, lo:lo + n_virt])
            turned = jnp.dot(swap[...], jnp.concatenate(stack, axis=0), preferred_element_type=F32).astype(BF16)
            for k in range(n_occ):
                line = turned[k * n_occ:(k + 1) * n_occ]
                tr[k * n_virt + ab * n_occ:k * n_virt + (ab + 1) * n_occ, :] = line
                ta[ab * n_occ:(ab + 1) * n_occ, k * n_virt:(k + 1) * n_virt] = line

    def particle_hole(i):
        with jax.named_scope("ph_spread"):
            spread(i)
        with jax.named_scope("ph_r5"):
            r5[...] = jnp.dot(wxt[...], tr[...], preferred_element_type=F32)
        with jax.named_scope("ph_r3"):
            r3[...] = jnp.dot(ta[...], wd[...], preferred_element_type=F32)
        with jax.named_scope("ph_diff"):
            for j in range(occ):
                diff = r3[:, j * n_virt:(j + 1) * n_virt] - r5[j * n_virt:(j + 1) * n_virt, :]
                sd[i * occ + j] = diff
                sp[j * occ + i] = diff.T

    @pl.loop(0, NQ + 1)
    def _(q):
        @pl.when(q < NQ)
        def _():
            send_z(q).wait_recv()

            @pl.when(jnp.logical_not(own_ladder))
            def _():
                send_lx(q).start()

            send_y(q).wait_recv()

            @pl.when(q == OVER_Y)
            def _():
                send_dy(q).start()

            @pl.when(q != OVER_Y)
            def _():
                send_dz(q).start()

        @pl.when(q + AHEAD < NQ)
        def _():
            send_y(q + AHEAD).start()
            send_z(q + AHEAD).start()

            @pl.when(own_ladder)
            def _():
                send_lx(q + AHEAD).start()

        @pl.when(q + 1 < NQ)
        def _():
            send_row(q + 1).start()

        for at, pieces in FORWARD:
            @pl.when(q == at)
            def _():
                for w in pieces:
                    forward_ladder(w)

        @pl.when(q >= 1)
        def _():
            send_dz(q - 1).wait_recv()
            particle_hole(q - 1)

    lad_p = remote(rows.at[r_p], lad.at[r], g_sem.at[0, 3], g_sem.at[1, 3], r_p, c)
    lad_p.start()
    lad[r] = rows[r]

    n_pair = occ * occ
    pad = pl.ds(cols_dev - tail, LANES)
    for k in range(n_col):
        msg_p[k, :, pad] = jnp.zeros((n_pair, LANES), F32)
        msg_d[k, :, pad] = jnp.zeros((n_pair, LANES), F32)
        part[k, :, pad] = jnp.zeros((rows_dev, LANES), F32)

    @pl.loop(0, n_col)
    def _(k):
        for a in range(vir):
            msg_p[k, :, a * n_virt:(a + 1) * n_virt] = sp[:, k * vir + a, :]

    def p_send(off, width, n, k, p):
        at = pl.ds(off, width)
        return remote(msg_p.at[p, :, at], got_p.at[c, :, at], ps_sem.at[k, n], pr_sem.at[k, n], r, p)

    chunks = [(n * CHUNK, CHUNK) for n in range(n_full)] + [(n_full * CHUNK, LANES)]
    for n, (off, width) in enumerate(chunks[:P_AHEAD]):
        for k, p in enumerate(col_peers):
            p_send(off, width, n, k, p).start()
    own_p = pltpu.make_async_copy(msg_p.at[c], got_p.at[c], loc_sem.at[0])
    own_p.start()

    def d_send(k, p):
        return remote(msg_d.at[p], got_d.at[c], d_sem.at[0, k], d_sem.at[1, k], r, p)

    own_d = pltpu.make_async_copy(msg_d.at[c], got_d.at[c], loc_sem.at[1])

    def form_d():
        @pl.loop(0, n_col)
        def _(k):
            for a in range(vir):
                msg_d[k, :, a * n_virt:(a + 1) * n_virt] = sd[:, k * vir + a, :]

        for k, p in enumerate(col_peers):
            d_send(k, p).start()
        own_d.start()

    lad_p.wait_recv()

    @pl.when(jnp.logical_not(direct))
    def _():
        for q in range(NQ):
            for w in range(2):
                send_ly(w, q).wait_recv()

    @pl.when(direct)
    def _():
        for q in range(NQ):
            for w in range(2):
                send_ly(w, q).wait_send()
    lad_p.wait_send()
    ld_perm.wait()

    @pl.loop(0, n_row)
    def _(k):
        for off in range(0, cols_dev, CHUNK):
            width = min(CHUNK, cols_dev - off)
            block = jnp.dot(perm[...], lad[k, :, off:off + width], preferred_element_type=F32)
            lad[k, :, off:off + width] = block.astype(BF16)

    own_p.wait()

    for q in range(NQ):
        send_row(q).wait_recv()
    row_o.start()

    def h_send(off, width, n, w):
        at = pl.ds(off, width)
        return remote(part.at[2 * w + 1 - u, :, at], half.at[w, :, at], hs_sem.at[w, n], hr_sem.at[w, n], r_p, c)

    def x_pass(off, width, n):
        at = pl.ds(off, width)
        return remote(xsend.at[:, at], xgot.at[:, at], xs_sem.at[n], xr_sem.at[n], r_s, c)

    def across(off, width, n):
        at = pl.ds(off, width)
        with jax.named_scope("ph_wait_h"):
            for w in range(2):
                h_send(off, width, n, w).wait_recv()
        xsend[:, at] = part[2 * (1 - x) + u, :, at] + half[1 - x, :, at]
        x_pass(off, width, n).start()

    def ladder(off, width, n, v_ref):
        at = pl.ds(off, width)
        with jax.named_scope("ph_dot"):
            t_all = lad[...].reshape(n_row * rows_dev, cols_dev)
            prod = jnp.dot(t_all, v_ref[:, 0:min(width, cols_dev - off) if width == LANES else width], preferred_element_type=F32)
            part[:, :, pl.ds(off, prod.shape[1])] = prod.reshape(n_row, rows_dev, prod.shape[1])
        with jax.named_scope("ph_wait_p"):
            for k, p in enumerate(col_peers):
                p_send(off, width, n, k, p).wait_recv()
        mine = pl.ds(pl.multiple_of(r * n_pair, n_pair), n_pair)
        for k in range(n_col):
            part[k, mine, at] += got_p[k, :, at]
        for w in range(2):
            h_send(off, width, n, w).start()

    def x_send(k, p):
        return remote(xpart, xgot_part.at[c], x_sem.at[0, k], x_sem.at[1, k], r, p)

    def form_x():
        row_p.wait_recv()
        row_o.wait_recv()
        ld_oovv.wait()
        for k in range(n_row):
            xpart[:, k * rows_dev:(k + 1) * rows_dev] = lax.dot_general(
                oovv[...], tcols[k], (((1,), (1,)), ((), ())), preferred_element_type=F32)
        for k, p in enumerate(col_peers):
            x_send(k, p).start()

    def m_send(k, p):
        return remote(m_mine.at[p], m_got.at[r], m_sem.at[0, k], m_sem.at[1, k], p, c)

    def form_m():
        for k, p in enumerate(col_peers):
            x_send(k, p).wait_recv()
        xgot_part[c] = xpart[...]
        x_sum = xgot_part[0] + xgot_part[1] + xgot_part[2] + xgot_part[3]
        ld_oooo.wait()
        hole = (oooo[pl.ds(pl.multiple_of(r * rows_dev, rows_dev), rows_dev), :].astype(F32) + 0.5 * x_sum)
        for k in range(n_row):
            m_mine[k] = hole[:, k * rows_dev:(k + 1) * rows_dev].astype(BF16)
        for k, p in enumerate(row_peers):
            m_send(k, p).start()
        m_got[r] = m_mine[r]

    @pl.loop(0, n_full)
    def _(n):
        off = pl.multiple_of(n * CHUNK, CHUNK)
        with jax.named_scope("ph_wait_v"):
            fetch(off, CHUNK, n % 2).wait()
        ladder(off, CHUNK, n, vbuf.at[n % 2])

        @pl.when(n + 2 < n_full)
        def _():
            fetch(pl.multiple_of((n + 2) * CHUNK, CHUNK), CHUNK, n % 2).start()

        @pl.when(n + P_AHEAD < n_full)
        def _():
            later = pl.multiple_of((n + P_AHEAD) * CHUNK, CHUNK)
            for k, p in enumerate(col_peers):
                p_send(later, CHUNK, n + P_AHEAD, k, p).start()

        @pl.when(n + P_AHEAD == n_full)
        def _():
            for k, p in enumerate(col_peers):
                p_send(n_full * CHUNK, LANES, n_full, k, p).start()

        @pl.when(n == 2)
        def _():
            with jax.named_scope("ph_form_x"):
                form_x()

        @pl.when(n == 5)
        def _():
            with jax.named_scope("ph_form_m"):
                form_m()

        @pl.when(n == 7)
        def _():
            with jax.named_scope("ph_form_d"):
                form_d()

        @pl.when(n >= 1)
        def _():
            across(pl.multiple_of((n - 1) * CHUNK, CHUNK), CHUNK, n - 1)

    ladder(n_full * CHUNK, LANES, n_full, vlast)
    across((n_full - 1) * CHUNK, CHUNK, n_full - 1)
    across(n_full * CHUNK, LANES, n_full)

    for k, p in enumerate(row_peers):
        m_send(k, p).wait_recv()
    for k, p in enumerate(col_peers):
        d_send(k, p).wait_recv()
    own_d.wait()
    ld_den.wait()

    def finish(off, width, n):
        at = pl.ds(off, width)
        hole_term = None
        for k in range(n_row):
            term = lax.dot_general(
                m_got[k], tcols[k, :, at], (((0,), (0,)), ((), ())), preferred_element_type=F32)
            hole_term = term if hole_term is None else hole_term + term
        own = part[r, :, at] + half[x, :, at] + xgot[:, at]
        for jh in range(n_col):
            v = own[jh * n_pair:(jh + 1) * n_pair] + got_d[jh, :, at]
            for i in range(occ):
                lo = i * n_occ + jh * occ
                xgot[lo:lo + occ, at] = v[i * occ:(i + 1) * occ]
        total = oovv[:, at].astype(F32) + xgot[:, at] + hole_term
        t32[:, at] = total / t32[:, at]

    @pl.loop(0, n_full)
    def _(n):
        off = pl.multiple_of(n * CHUNK, CHUNK)
        x_pass(off, CHUNK, n).wait_recv()
        finish(off, CHUNK, n)

    x_pass(n_full * CHUNK, LANES, n_full).wait_recv()
    finish(n_full * CHUNK, tail, n_full)
    st = pltpu.make_async_copy(t32, out_hbm, in_sem.at[8])
    st.start()

    for q in range(NQ):
        send_y(q).wait_send()
        send_z(q).wait_send()
        send_dz(q).wait_send()
        send_row(q).wait_send()
        send_lx(q).wait_send()
    row_p.wait_send()
    row_o.wait_send()
    for k, p in enumerate(row_peers):
        m_send(k, p).wait_send()
    for k, p in enumerate(col_peers):
        x_send(k, p).wait_send()
        d_send(k, p).wait_send()
    for n, (off, width) in enumerate(chunks):
        for k, p in enumerate(col_peers):
            p_send(off, width, n, k, p).wait_send()
        for w in range(2):
            h_send(off, width, n, w).wait_send()
        x_pass(off, width, n).wait_send()
    st.wait()


def solution(mesh):
    n_row = mesh.shape["row"]
    n_col = mesh.shape["col"]
    amp_spec = P("row", "col")
    wide_spec = P(None, "col")

    def local_sweep(t_blk, d_blk, oovv_blk, vvvv_blk, oooo_full, wd_blk, wx_blk):
        rows_dev, cols_dev = t_blk.shape
        n_occ = math.isqrt(oooo_full.shape[0])
        n_virt = wd_blk.shape[0] // n_occ
        occ, vir = n_occ // n_row, n_virt // n_col
        n_pair = occ * occ
        n_chunk = cols_dev // CHUNK + 1
        wide = -(-cols_dev // LANES) * LANES
        kc, jb = wd_blk.shape
        perm = np.eye(rows_dev, dtype=BF16).reshape(occ, n_col, occ, rows_dev).transpose(1, 0, 2, 3).reshape(rows_dev, rows_dev)
        n_sq = n_occ * n_occ
        swap = np.eye(n_sq, dtype=BF16).reshape(n_occ, n_occ, n_sq).transpose(1, 0, 2).reshape(n_sq, n_sq)
        dma = pltpu.SemaphoreType.DMA
        vm = pltpu.VMEM
        hbm = pl.BlockSpec(memory_space=pl.ANY)
        block = (rows_dev, cols_dev)
        return pl.pallas_call(
            functools.partial(sweep_kernel, (n_occ, n_virt, n_row, n_col)),
            out_shape=jax.ShapeDtypeStruct(block, F32),
            grid=(1,),
            in_specs=[hbm] * 4 + [pl.BlockSpec((cols_dev, LANES), lambda i: (0, cols_dev // LANES), pipeline_mode=pl.Buffered(1))] + [hbm] * 5,
            out_specs=hbm,
            scratch_shapes=[
                vm(block, F32), vm((n_col,) + block, BF16), vm((n_row,) + block, BF16), vm((n_row,) + block, BF16),
                vm((kc, jb), BF16), vm((jb, kc), BF16), vm((jb, kc), BF16),
                vm((kc, n_virt), BF16), vm((n_virt, kc), BF16), vm((n_virt, jb), F32), vm((jb, n_virt), F32),
                vm((n_pair, n_virt, n_virt), F32), vm((n_pair, n_virt, n_virt), F32),
                vm((n_col, n_pair, wide), F32), vm((n_col, n_pair, wide), F32),
                vm((n_col, n_pair, wide), F32), vm((n_col, n_pair, wide), F32),
                vm((n_row, rows_dev, wide), F32), vm((2, rows_dev, wide), F32),
                vm((rows_dev, wide), F32), vm((rows_dev, wide), F32),
                vm((2, cols_dev, CHUNK), BF16), vm(block, BF16), vm(oooo_full.shape, BF16),
                vm((rows_dev, rows_dev), BF16), vm((n_sq, n_sq), BF16),
                vm((rows_dev, n_sq), F32), vm((n_col, rows_dev, n_sq), F32),
                vm((n_row, rows_dev, rows_dev), BF16), vm((n_row, rows_dev, rows_dev), BF16),
                dma((10,)), dma((2,)), dma((2,)), dma((3, NQ)), dma((3, NQ)), dma((3, NQ)), dma((4, NQ)), dma((2, 4)),
                dma((2, NQ)), dma((3, n_chunk)), dma((3, n_chunk)), dma((2, 3)), dma((2, n_chunk)), dma((2, n_chunk)),
                dma((n_chunk,)), dma((n_chunk,)), dma((2, 3)), dma((2, 3)),
            ],
            compiler_params=pltpu.CompilerParams(
                collective_id=0, has_side_effects=True, vmem_limit_bytes=67043328),
        )(t_blk, d_blk, oovv_blk, vvvv_blk, vvvv_blk, oooo_full, wd_blk.T, wx_blk.T, jnp.asarray(perm), jnp.asarray(swap))

    return jax.shard_map(
        local_sweep, mesh=mesh,
        in_specs=(amp_spec, amp_spec, amp_spec, amp_spec, P(), wide_spec, wide_spec),
        out_specs=amp_spec, check_vma=False)
```

```python
import functools
import math

import jax
import jax.numpy as jnp
import numpy as np
from jax import lax
from jax.experimental import pallas as pl
from jax.experimental.pallas import tpu as pltpu
from jax.sharding import PartitionSpec as P

F32 = jnp.float32
BF16 = jnp.bfloat16
MESH = pl.DeviceIdType.MESH
CHUNK = 512
LANES = 128
D_FIRST, D_SECOND = 5, 7
P_AHEAD = 6
AHEAD = 2
OVER_Y = 1
NQ = 4


def sweep_kernel(
    dims,
    t_hbm, den_hbm, oovv_hbm, vvvv_hbm, vlast, oooo_hbm, wd_hbm, wx_hbm, perm_hbm, swap_hbm,
    out,
    t32, rows, lad, tcols, wd, wdt, wxt, tr, ta, r3, r5, sd, sp, msg_d, msg_p, got_d, got_p,
    part, half, xsend, xgot, turned, vbuf, oovv, oooo, perm, swap, xpart, xgot_part, m_mine, m_got,
    in_sem, vb_sem, loc_sem, ts_sem, tr_sem, ls_sem, lr_sem, g_sem,
    rx_sem, ps_sem, pr_sem, d_sem, hs_sem, hr_sem, xs_sem, xr_sem, x_sem, m_sem,
):
    n_occ, n_virt, n_row, n_col = dims
    rows_dev, cols_dev = t32.shape
    occ = n_occ // n_row
    vir = n_virt // n_col
    qrows = rows_dev // NQ
    n_full = cols_dev // CHUNK
    tail = cols_dev - n_full * CHUNK
    r = lax.axis_index("row")
    c = lax.axis_index("col")
    x, u = r // 2, r % 2
    z, y = c // 2, c % 2
    c_y, c_z, c_d = 2 * z + 1 - y, 2 * (1 - z) + y, 2 * (1 - z) + 1 - y
    r_p, r_s, r_o = 2 * x + 1 - u, 2 * (1 - x) + u, 2 * (1 - x) + 1 - u
    col_peers = (c_y, c_z, c_d)
    row_peers = (r_p, r_s, r_o)

    def remote(src, dst, ssem, rsem, row, col):
        return pltpu.make_async_remote_copy(
            src_ref=src, dst_ref=dst, send_sem=ssem, recv_sem=rsem,
            device_id={"row": row, "col": col}, device_id_type=MESH)

    def load(src, dst, k):
        return pltpu.make_async_copy(src, dst, in_sem.at[k])

    ld_t = load(t_hbm, t32, 0)
    ld_wx = load(wx_hbm, wxt, 1)
    ld_wd = load(wd_hbm, wdt, 2)
    ld_oovv = load(oovv_hbm, oovv, 3)
    ld_oooo = load(oooo_hbm, oooo, 4)
    ld_perm = load(perm_hbm, perm, 5)
    ld_swap = load(swap_hbm, swap, 6)
    ld_den = load(den_hbm, t32, 7)
    for ld in (ld_t, ld_wx, ld_wd, ld_oovv, ld_oooo, ld_perm, ld_swap):
        ld.start()

    def fetch(off, width, slot):
        return pltpu.make_async_copy(vvvv_hbm.at[:, pl.ds(off, width)], vbuf.at[slot], vb_sem.at[slot])

    for s in range(2):
        fetch(s * CHUNK, CHUNK, s).start()

    barrier = pltpu.get_barrier_semaphore()
    for p in col_peers:
        pl.semaphore_signal(barrier, inc=1, device_id={"row": r, "col": p}, device_id_type=MESH)
    for p in row_peers:
        pl.semaphore_signal(barrier, inc=1, device_id={"row": p, "col": c}, device_id_type=MESH)
    pl.semaphore_wait(barrier, 6)

    def piece(ref, k, q):
        return ref.at[k, pl.ds(pl.multiple_of(q * qrows, qrows), qrows), :]

    def send_y(q):
        return remote(piece(rows, c, q), piece(rows, c, q), ts_sem.at[0, q], tr_sem.at[0, q], r, c_y)

    def send_z(q):
        return remote(piece(rows, c, q), piece(rows, c, q), ts_sem.at[1, q], tr_sem.at[1, q], r, c_z)

    def send_dz(q):
        return remote(piece(rows, c_y, q), piece(rows, c_y, q), ts_sem.at[2, q], tr_sem.at[2, q], r, c_z)

    def send_dy(q):
        return remote(piece(rows, c_z, q), piece(rows, c_z, q), ts_sem.at[2, q], tr_sem.at[2, q], r, c_y)

    blk_x = 2 * (1 - x) + y

    def send_lx(q):
        return remote(piece(rows, blk_x, q), piece(lad, r, q), ls_sem.at[0, q], lr_sem.at[u, q], blk_x, c)

    def recv_lx(w, q):
        k = 2 * (1 - x) + w
        return remote(piece(lad, k, q), piece(lad, k, q), ls_sem.at[0, q], lr_sem.at[w, q], blk_x, c)

    def send_ly(w, q):
        k = 2 * (1 - x) + w
        return remote(piece(lad, k, q), piece(lad, k, q), ls_sem.at[1 + w, q], lr_sem.at[2 + w, q], r, c_y)

    own_ladder = z == 1 - x
    direct = u == y

    ld_t.wait()
    for q in range(NQ):
        rows[c, pl.ds(q * qrows, qrows), :] = t32[pl.ds(q * qrows, qrows), :].astype(BF16)
        if q < AHEAD:
            send_y(q).start()
            send_z(q).start()

            @pl.when(own_ladder)
            def _():
                send_lx(q).start()

    ld_den.start()

    def send_row(q):
        return remote(piece(rows, c, q), piece(tcols, r, q), rx_sem.at[0, q], rx_sem.at[1, q], r_s, c)

    row_p = remote(rows.at[c], tcols.at[r], g_sem.at[0, 0], g_sem.at[1, 0], r_p, c)
    row_o = remote(tcols.at[r_s], tcols.at[r_s], g_sem.at[0, 1], g_sem.at[1, 1], r_p, c)
    row_p.start()
    send_row(0).start()
    tcols[r] = rows[c]

    with jax.named_scope("ph_turn_w"):
        ld_wd.wait()

        @pl.loop(0, wd.shape[0] // LANES)
        def _(m):
            at = pl.ds(pl.multiple_of(m * LANES, LANES), LANES)
            for b in range(0, wd.shape[1], LANES):
                w = min(LANES, wd.shape[1] - b)
                wd[at, b:b + w] = wdt[b:b + w, at].astype(F32).T.astype(BF16)

    def forward_ladder(q):
        @pl.when(direct)
        def _():
            for w in range(2):
                recv_lx(w, q).wait_recv()
                send_ly(w, q).start()

    ld_swap.wait()
    ld_wx.wait()

    def spread(i):
        lines = pl.ds(pl.multiple_of(i * n_occ, n_occ), n_occ)
        for ab in range(n_virt // n_occ):
            stack = []
            for t in range(n_occ):
                a = ab * n_occ + t
                lo = (a % vir) * n_virt
                stack.append(rows[a // vir, lines, lo:lo + n_virt])
            lines_k = jnp.dot(swap[...], jnp.concatenate(stack, axis=0), preferred_element_type=F32).astype(BF16)
            for k in range(n_occ):
                line = lines_k[k * n_occ:(k + 1) * n_occ]
                tr[k * n_virt + ab * n_occ:k * n_virt + (ab + 1) * n_occ, :] = line
                ta[ab * n_occ:(ab + 1) * n_occ, k * n_virt:(k + 1) * n_virt] = line

    def particle_hole(i, between):
        with jax.named_scope("ph_spread"):
            spread(i)
        with jax.named_scope("ph_r5"):
            r5[...] = jnp.dot(wxt[...], tr[...], preferred_element_type=F32)
        between()
        with jax.named_scope("ph_r3"):
            r3[...] = jnp.dot(ta[...], wd[...], preferred_element_type=F32)
        with jax.named_scope("ph_diff"):
            for j in range(occ):
                diff = r3[:, j * n_virt:(j + 1) * n_virt] - r5[j * n_virt:(j + 1) * n_virt, :]
                sd[i * occ + j] = diff
                sp[j * occ + i] = diff.T

    def stage(q):
        send_z(q).wait_recv()

        @pl.when(jnp.logical_not(own_ladder))
        def _():
            send_lx(q).start()

        send_y(q).wait_recv()

        @pl.when(q == OVER_Y)
        def _():
            send_dy(q).start()

        @pl.when(q != OVER_Y)
        def _():
            send_dz(q).start()

        @pl.when(q + AHEAD < NQ)
        def _():
            send_y(q + AHEAD).start()
            send_z(q + AHEAD).start()

            @pl.when(own_ladder)
            def _():
                send_lx(q + AHEAD).start()

    def on_step(q, step, act, *args):
        @pl.when(q == step)
        def _():
            act(*args)

    def go_row(q):
        send_row(q).start()

    with jax.named_scope("ph_stages"):
        stage(0)
        stage(1)
        go_row(1)

    @pl.loop(0, NQ)
    def _(q):
        send_dz(q).wait_recv()
        on_step(q, 0, go_row, 2)
        on_step(q, 1, forward_ladder, 0)
        on_step(q, 3, forward_ladder, 3)

        def between():
            @pl.when(q + 2 < NQ)
            def _():
                stage(q + 2)

            on_step(q, 1, forward_ladder, 1)
            on_step(q, 2, forward_ladder, 2)
            on_step(q, 2, go_row, 3)

        particle_hole(q, between)

    lad_p = remote(rows.at[r_p], lad.at[r], g_sem.at[0, 3], g_sem.at[1, 3], r_p, c)
    lad_p.start()
    lad[r] = rows[r]

    n_pair = occ * occ
    pad = pl.ds(cols_dev - tail, LANES)
    for k in range(n_col):
        msg_p[k, :, pad] = jnp.zeros((n_pair, LANES), F32)
        msg_d[k, :, pad] = jnp.zeros((n_pair, LANES), F32)
        part[k, :, pad] = jnp.zeros((rows_dev, LANES), F32)

    @pl.loop(0, n_col)
    def _(k):
        for a in range(vir):
            msg_p[k, :, a * n_virt:(a + 1) * n_virt] = sp[:, k * vir + a, :]

    def p_send(off, width, n, k, p):
        at = pl.ds(off, width)
        return remote(msg_p.at[p, :, at], got_p.at[c, :, at], ps_sem.at[k, n], pr_sem.at[k, n], r, p)

    chunks = [(n * CHUNK, CHUNK) for n in range(n_full)] + [(n_full * CHUNK, LANES)]
    for n, (off, width) in enumerate(chunks[:P_AHEAD]):
        for k, p in enumerate(col_peers):
            p_send(off, width, n, k, p).start()
    own_p = pltpu.make_async_copy(msg_p.at[c], got_p.at[c], loc_sem.at[0])
    own_p.start()

    d_cut = n_full // 2 * CHUNK
    d_halves = ((0, d_cut), (d_cut, msg_d.shape[2] - d_cut))

    def d_send(w, k, p):
        at = pl.ds(*d_halves[w])
        return remote(msg_d.at[p, :, at], got_d.at[c, :, at], d_sem.at[0, w, k], d_sem.at[1, w, k], r, p)

    own_d = pltpu.make_async_copy(msg_d.at[c], got_d.at[c], loc_sem.at[1])

    def go_d(w):
        for k, p in enumerate(col_peers):
            d_send(w, k, p).start()

    def form_d():
        @pl.loop(0, n_col)
        def _(k):
            for a in range(vir):
                msg_d[k, :, a * n_virt:(a + 1) * n_virt] = sd[:, k * vir + a, :]

        go_d(0)
        own_d.start()

    lad_p.wait_recv()

    @pl.when(jnp.logical_not(direct))
    def _():
        for q in range(NQ):
            for w in range(2):
                send_ly(w, q).wait_recv()

    @pl.when(direct)
    def _():
        for q in range(NQ):
            for w in range(2):
                send_ly(w, q).wait_send()
    lad_p.wait_send()
    ld_perm.wait()

    @pl.loop(0, n_row)
    def _(k):
        for off in range(0, cols_dev, CHUNK):
            width = min(CHUNK, cols_dev - off)
            block = jnp.dot(perm[...], lad[k, :, off:off + width], preferred_element_type=F32)
            lad[k, :, off:off + width] = block.astype(BF16)

    own_p.wait()

    for q in range(NQ):
        send_row(q).wait_recv()
    row_o.start()

    def h_send(off, width, n, w):
        at = pl.ds(off, width)
        return remote(part.at[2 * w + 1 - u, :, at], half.at[w, :, at], hs_sem.at[w, n], hr_sem.at[w, n], r_p, c)

    def x_pass(off, width, n):
        return remote(xsend.at[n, :, pl.ds(0, width)], xgot.at[n, :, pl.ds(0, width)], xs_sem.at[n], xr_sem.at[n], r_s, c)

    def across(off, width, n):
        at = pl.ds(off, width)
        with jax.named_scope("ph_wait_h"):
            for w in range(2):
                h_send(off, width, n, w).wait_recv()
        xsend[n, :, 0:width] = part[2 * (1 - x) + u, :, at] + half[1 - x, :, at]
        x_pass(off, width, n).start()

    def ladder(off, width, n, v_ref):
        at = pl.ds(off, width)
        with jax.named_scope("ph_dot"):
            t_all = lad[...].reshape(n_row * rows_dev, cols_dev)
            prod = jnp.dot(t_all, v_ref[:, 0:min(width, cols_dev - off) if width == LANES else width], preferred_element_type=F32)
            part[:, :, pl.ds(off, prod.shape[1])] = prod.reshape(n_row, rows_dev, prod.shape[1])
        with jax.named_scope("ph_wait_p"):
            for k, p in enumerate(col_peers):
                p_send(off, width, n, k, p).wait_recv()
        mine = pl.ds(pl.multiple_of(r * n_pair, n_pair), n_pair)
        for k in range(n_col):
            part[k, mine, at] += got_p[k, :, at]
        for w in range(2):
            h_send(off, width, n, w).start()

    def x_send(k, p):
        return remote(xpart, xgot_part.at[c], x_sem.at[0, k], x_sem.at[1, k], r, p)

    def form_x():
        row_p.wait_recv()
        row_o.wait_recv()
        ld_oovv.wait()
        for k in range(n_row):
            xpart[:, k * rows_dev:(k + 1) * rows_dev] = lax.dot_general(
                oovv[...], tcols[k], (((1,), (1,)), ((), ())), preferred_element_type=F32)
        for k, p in enumerate(col_peers):
            x_send(k, p).start()

    def m_send(k, p):
        return remote(m_mine.at[p], m_got.at[r], m_sem.at[0, k], m_sem.at[1, k], p, c)

    def form_m():
        for k, p in enumerate(col_peers):
            x_send(k, p).wait_recv()
        xgot_part[c] = xpart[...]
        x_sum = xgot_part[0] + xgot_part[1] + xgot_part[2] + xgot_part[3]
        ld_oooo.wait()
        hole = (oooo[pl.ds(pl.multiple_of(r * rows_dev, rows_dev), rows_dev), :].astype(F32) + 0.5 * x_sum)
        for k in range(n_row):
            m_mine[k] = hole[:, k * rows_dev:(k + 1) * rows_dev].astype(BF16)
        for k, p in enumerate(row_peers):
            m_send(k, p).start()
        m_got[r] = m_mine[r]

    @pl.loop(0, n_full)
    def _(n):
        off = pl.multiple_of(n * CHUNK, CHUNK)
        with jax.named_scope("ph_wait_v"):
            fetch(off, CHUNK, n % 2).wait()
        ladder(off, CHUNK, n, vbuf.at[n % 2])

        @pl.when(n + 2 < n_full)
        def _():
            fetch(pl.multiple_of((n + 2) * CHUNK, CHUNK), CHUNK, n % 2).start()

        @pl.when(n + P_AHEAD < n_full)
        def _():
            later = pl.multiple_of((n + P_AHEAD) * CHUNK, CHUNK)
            for k, p in enumerate(col_peers):
                p_send(later, CHUNK, n + P_AHEAD, k, p).start()

        @pl.when(n + P_AHEAD == n_full)
        def _():
            for k, p in enumerate(col_peers):
                p_send(n_full * CHUNK, LANES, n_full, k, p).start()

        @pl.when(n == 2)
        def _():
            with jax.named_scope("ph_form_x"):
                form_x()

        @pl.when(n == 8)
        def _():
            with jax.named_scope("ph_form_m"):
                form_m()

        @pl.when(n == D_FIRST)
        def _():
            with jax.named_scope("ph_form_d"):
                form_d()

        @pl.when(n == D_SECOND)
        def _():
            go_d(1)

        @pl.when(n >= 1)
        def _():
            across(pl.multiple_of((n - 1) * CHUNK, CHUNK), CHUNK, n - 1)

    ladder(n_full * CHUNK, LANES, n_full, vlast)
    across((n_full - 1) * CHUNK, CHUNK, n_full - 1)
    across(n_full * CHUNK, LANES, n_full)

    with jax.named_scope("ph_fin_m"):
        for k, p in enumerate(row_peers):
            m_send(k, p).wait_recv()
    ld_den.wait()

    def hole_term(off, width):
        at = pl.ds(off, width)
        total = None
        for k in range(n_row):
            term = lax.dot_general(
                m_got[k], tcols[k, :, at], (((0,), (0,)), ((), ())), preferred_element_type=F32)
            total = term if total is None else total + term
        part[r_s, :, at] = total + oovv[:, at].astype(F32)
        part[r, :, pl.ds(off, width)] += half[x, :, at]

    def finish(off, width, n):
        at = pl.ds(off, width)
        own = part[r, :, at] + xgot[n, :, 0:width]
        for jh in range(n_col):
            v = own[jh * n_pair:(jh + 1) * n_pair] + got_d[jh, :, at]
            for i in range(occ):
                lo = i * n_occ + jh * occ
                turned[lo:lo + occ, 0:width] = v[i * occ:(i + 1) * occ]
        out[:, at] = (part[r_s, :, at] + turned[:, 0:width]) / t32[:, at]

    def full(n):
        return pl.multiple_of(n * CHUNK, CHUNK)

    @pl.loop(0, n_full)
    def _(n):
        hole_term(full(n), CHUNK)

    hole_term(n_full * CHUNK, tail)
    n_cut = d_cut // CHUNK

    def wait_d(w):
        with jax.named_scope("ph_fin_d"):
            for k, p in enumerate(col_peers):
                d_send(w, k, p).wait_recv()

    own_d.wait()
    wait_d(0)

    @pl.loop(0, n_full)
    def _(n):
        @pl.when(n == n_cut)
        def _():
            wait_d(1)

        with jax.named_scope("ph_fin_x"):
            x_pass(full(n), CHUNK, n).wait_recv()
        finish(full(n), CHUNK, n)

    x_pass(n_full * CHUNK, LANES, n_full).wait_recv()
    finish(n_full * CHUNK, tail, n_full)

    for q in range(NQ):
        send_y(q).wait_send()
        send_z(q).wait_send()
        send_dz(q).wait_send()
        send_row(q).wait_send()
        send_lx(q).wait_send()
    row_p.wait_send()
    row_o.wait_send()
    for k, p in enumerate(row_peers):
        m_send(k, p).wait_send()
    for k, p in enumerate(col_peers):
        x_send(k, p).wait_send()
        for w in range(2):
            d_send(w, k, p).wait_send()
    for n, (off, width) in enumerate(chunks):
        for k, p in enumerate(col_peers):
            p_send(off, width, n, k, p).wait_send()
        for w in range(2):
            h_send(off, width, n, w).wait_send()
        x_pass(off, width, n).wait_send()


def solution(mesh):
    n_row = mesh.shape["row"]
    n_col = mesh.shape["col"]
    amp_spec = P("row", "col")
    wide_spec = P(None, "col")

    def local_sweep(t_blk, d_blk, oovv_blk, vvvv_blk, oooo_full, wd_blk, wx_blk):
        rows_dev, cols_dev = t_blk.shape
        n_occ = math.isqrt(oooo_full.shape[0])
        n_virt = wd_blk.shape[0] // n_occ
        occ, vir = n_occ // n_row, n_virt // n_col
        n_pair = occ * occ
        n_chunk = cols_dev // CHUNK + 1
        wide = -(-cols_dev // LANES) * LANES
        kc, jb = wd_blk.shape
        perm = np.eye(rows_dev, dtype=BF16).reshape(occ, n_col, occ, rows_dev).transpose(1, 0, 2, 3).reshape(rows_dev, rows_dev)
        n_sq = n_occ * n_occ
        swap = np.eye(n_sq, dtype=BF16).reshape(n_occ, n_occ, n_sq).transpose(1, 0, 2).reshape(n_sq, n_sq)
        dma = pltpu.SemaphoreType.DMA
        vm = pltpu.VMEM
        hbm = pl.BlockSpec(memory_space=pl.ANY)
        block = (rows_dev, cols_dev)
        return pl.pallas_call(
            functools.partial(sweep_kernel, (n_occ, n_virt, n_row, n_col)),
            out_shape=pltpu.VMEM(block, F32),
            grid=(1,),
            in_specs=[hbm] * 4 + [pl.BlockSpec((cols_dev, LANES), lambda i: (0, cols_dev // LANES), pipeline_mode=pl.Buffered(1))] + [hbm] * 5,
            out_specs=pl.BlockSpec(memory_space=pltpu.VMEM),
            scratch_shapes=[
                vm(block, F32), vm((n_col,) + block, BF16), vm((n_row,) + block, BF16), vm((n_row,) + block, BF16),
                vm((kc, jb), BF16), vm((jb, kc), BF16), vm((jb, kc), BF16),
                vm((kc, n_virt), BF16), vm((n_virt, kc), BF16), vm((n_virt, jb), F32), vm((jb, n_virt), F32),
                vm((n_pair, n_virt, n_virt), F32), vm((n_pair, n_virt, n_virt), F32),
                vm((n_col, n_pair, wide), F32), vm((n_col, n_pair, wide), F32),
                vm((n_col, n_pair, wide), F32), vm((n_col, n_pair, wide), F32),
                vm((n_row, rows_dev, wide), F32), vm((2, rows_dev, wide), F32),
                vm((n_chunk, rows_dev, CHUNK), F32), vm((n_chunk, rows_dev, CHUNK), F32), vm((rows_dev, CHUNK), F32),
                vm((2, cols_dev, CHUNK), BF16), vm(block, BF16), vm(oooo_full.shape, BF16),
                vm((rows_dev, rows_dev), BF16), vm((n_sq, n_sq), BF16),
                vm((rows_dev, n_sq), F32), vm((n_col, rows_dev, n_sq), F32),
                vm((n_row, rows_dev, rows_dev), BF16), vm((n_row, rows_dev, rows_dev), BF16),
                dma((10,)), dma((2,)), dma((2,)), dma((3, NQ)), dma((3, NQ)), dma((4, NQ)), dma((4, NQ)), dma((2, 4)),
                dma((2, NQ)), dma((3, n_chunk)), dma((3, n_chunk)), dma((2, 2, 3)), dma((2, n_chunk)), dma((2, n_chunk)),
                dma((n_chunk,)), dma((n_chunk,)), dma((2, 3)), dma((2, 3)),
            ],
            compiler_params=pltpu.CompilerParams(
                collective_id=0, has_side_effects=True, vmem_limit_bytes=65536000),
        )(t_blk, d_blk, oovv_blk, vvvv_blk, vvvv_blk, oooo_full, wd_blk.T, wx_blk.T, jnp.asarray(perm), jnp.asarray(swap))

    return jax.shard_map(
        local_sweep, mesh=mesh,
        in_specs=(amp_spec, amp_spec, amp_spec, amp_spec, P(), wide_spec, wide_spec),
        out_specs=amp_spec, check_vma=False)
```

```python
import functools
import math

import jax
import jax.numpy as jnp
import numpy as np
from jax import lax
from jax.experimental import pallas as pl
from jax.experimental.pallas import tpu as pltpu
from jax.sharding import PartitionSpec as P

F32 = jnp.float32
BF16 = jnp.bfloat16
MESH = pl.DeviceIdType.MESH
CHUNK = 512
LANES = 128
D_FIRST, D_SECOND = 5, 7
P_FIRST, P_AHEAD = 2, 6
AHEAD = 2
OVER_Y = 1
NQ = 4


def sweep_kernel(
    dims,
    t_hbm, den_hbm, oovv_hbm, vvvv_hbm, vlast, oooo_hbm, wd_hbm, wx_hbm, perm_hbm, swap_hbm,
    out,
    t32, rows, lad, tcols, wd, wdt, wxt, tr, ta, r3, r5, sd, sp, msg_d, msg_p, got_d, got_p,
    part, half, xsend, xgot, turned, vbuf, oovv, oooo, perm, swap, xpart, xgot_part, m_mine, m_got,
    in_sem, vb_sem, loc_sem, ts_sem, tr_sem, ls_sem, lr_sem, g_sem,
    rx_sem, ps_sem, pr_sem, d_sem, hs_sem, hr_sem, xs_sem, xr_sem, x_sem, m_sem,
):
    n_occ, n_virt, n_row, n_col = dims
    rows_dev, cols_dev = t32.shape
    occ = n_occ // n_row
    vir = n_virt // n_col
    qrows = rows_dev // NQ
    n_full = cols_dev // CHUNK
    tail = cols_dev - n_full * CHUNK
    r = lax.axis_index("row")
    c = lax.axis_index("col")
    x, u = r // 2, r % 2
    z, y = c // 2, c % 2
    c_y, c_z, c_d = 2 * z + 1 - y, 2 * (1 - z) + y, 2 * (1 - z) + 1 - y
    r_p, r_s, r_o = 2 * x + 1 - u, 2 * (1 - x) + u, 2 * (1 - x) + 1 - u
    col_peers = (c_y, c_z, c_d)
    row_peers = (r_p, r_s, r_o)

    def remote(src, dst, ssem, rsem, row, col):
        return pltpu.make_async_remote_copy(
            src_ref=src, dst_ref=dst, send_sem=ssem, recv_sem=rsem,
            device_id={"row": row, "col": col}, device_id_type=MESH)

    def load(src, dst, k):
        return pltpu.make_async_copy(src, dst, in_sem.at[k])

    ld_t = load(t_hbm, t32, 0)
    ld_wx = load(wx_hbm, wxt, 1)
    ld_wd = load(wd_hbm, wdt, 2)
    ld_oovv = load(oovv_hbm, oovv, 3)
    ld_oooo = load(oooo_hbm, oooo, 4)
    ld_perm = load(perm_hbm, perm, 5)
    ld_swap = load(swap_hbm, swap, 6)
    ld_den = load(den_hbm, t32, 7)
    for ld in (ld_t, ld_wx, ld_wd, ld_oovv, ld_oooo, ld_perm, ld_swap):
        ld.start()

    def fetch(off, width, slot):
        return pltpu.make_async_copy(vvvv_hbm.at[:, pl.ds(off, width)], vbuf.at[slot], vb_sem.at[slot])

    for s in range(2):
        fetch(s * CHUNK, CHUNK, s).start()

    barrier = pltpu.get_barrier_semaphore()
    for p in col_peers:
        pl.semaphore_signal(barrier, inc=1, device_id={"row": r, "col": p}, device_id_type=MESH)
    for p in row_peers:
        pl.semaphore_signal(barrier, inc=1, device_id={"row": p, "col": c}, device_id_type=MESH)
    pl.semaphore_wait(barrier, 6)

    def piece(ref, k, q):
        return ref.at[k, pl.ds(pl.multiple_of(q * qrows, qrows), qrows), :]

    def send_y(q):
        return remote(piece(rows, c, q), piece(rows, c, q), ts_sem.at[0, q], tr_sem.at[0, q], r, c_y)

    def send_z(q):
        return remote(piece(rows, c, q), piece(rows, c, q), ts_sem.at[1, q], tr_sem.at[1, q], r, c_z)

    def send_dz(q):
        return remote(piece(rows, c_y, q), piece(rows, c_y, q), ts_sem.at[2, q], tr_sem.at[2, q], r, c_z)

    def send_dy(q):
        return remote(piece(rows, c_z, q), piece(rows, c_z, q), ts_sem.at[2, q], tr_sem.at[2, q], r, c_y)

    blk_x = 2 * (1 - x) + y

    def send_lx(q):
        return remote(piece(rows, blk_x, q), piece(lad, r, q), ls_sem.at[0, q], lr_sem.at[u, q], blk_x, c)

    def recv_lx(w, q):
        k = 2 * (1 - x) + w
        return remote(piece(lad, k, q), piece(lad, k, q), ls_sem.at[0, q], lr_sem.at[w, q], blk_x, c)

    def send_ly(w, q):
        k = 2 * (1 - x) + w
        return remote(piece(lad, k, q), piece(lad, k, q), ls_sem.at[1 + w, q], lr_sem.at[2 + w, q], r, c_y)

    def send_lo(q):
        k = 2 * (1 - x) + 1 - y
        return remote(piece(rows, k, q), piece(lad, r, q), ls_sem.at[3, q], lr_sem.at[2 + u, q], k, c)

    def go_lo(q):
        send_lo(q).start()

    own_ladder = z == 1 - x
    direct = u == y

    ld_t.wait()
    for q in range(NQ):
        rows[c, pl.ds(q * qrows, qrows), :] = t32[pl.ds(q * qrows, qrows), :].astype(BF16)
        if q < AHEAD:
            send_y(q).start()
            send_z(q).start()

            @pl.when(own_ladder)
            def _():
                send_lx(q).start()

    ld_den.start()

    def send_row(q):
        return remote(piece(rows, c, q), piece(tcols, r, q), rx_sem.at[0, q], rx_sem.at[1, q], r_s, c)

    row_p = remote(rows.at[c], tcols.at[r], g_sem.at[0, 0], g_sem.at[1, 0], r_p, c)
    row_o = remote(tcols.at[r_s], tcols.at[r_s], g_sem.at[0, 1], g_sem.at[1, 1], r_p, c)
    row_p.start()
    send_row(0).start()
    tcols[r] = rows[c]

    with jax.named_scope("ph_turn_w"):
        ld_wd.wait()

        @pl.loop(0, wd.shape[0] // LANES)
        def _(m):
            at = pl.ds(pl.multiple_of(m * LANES, LANES), LANES)
            for b in range(0, wd.shape[1], LANES):
                w = min(LANES, wd.shape[1] - b)
                wd[at, b:b + w] = wdt[b:b + w, at].astype(F32).T.astype(BF16)

    def forward_ladder(q):
        @pl.when(direct)
        def _():
            for w in range(2):
                recv_lx(w, q).wait_recv()
                send_ly(w, q).start()

    ld_swap.wait()
    ld_wx.wait()

    def spread(i):
        lines = pl.ds(pl.multiple_of(i * n_occ, n_occ), n_occ)
        for ab in range(n_virt // n_occ):
            stack = []
            for t in range(n_occ):
                a = ab * n_occ + t
                lo = (a % vir) * n_virt
                stack.append(rows[a // vir, lines, lo:lo + n_virt])
            lines_k = jnp.dot(swap[...], jnp.concatenate(stack, axis=0), preferred_element_type=F32).astype(BF16)
            for k in range(n_occ):
                line = lines_k[k * n_occ:(k + 1) * n_occ]
                tr[k * n_virt + ab * n_occ:k * n_virt + (ab + 1) * n_occ, :] = line
                ta[ab * n_occ:(ab + 1) * n_occ, k * n_virt:(k + 1) * n_virt] = line

    def particle_hole(i, between):
        with jax.named_scope("ph_spread"):
            spread(i)
        with jax.named_scope("ph_r5"):
            r5[...] = jnp.dot(wxt[...], tr[...], preferred_element_type=F32)
            r3[...] = jnp.dot(ta[...], wd[...], preferred_element_type=F32)
        between()
        with jax.named_scope("ph_diff"):
            for j in range(occ):
                diff = r3[:, j * n_virt:(j + 1) * n_virt] - r5[j * n_virt:(j + 1) * n_virt, :]
                sd[i * occ + j] = diff
                sp[j * occ + i] = diff.T

    lad_p = remote(rows.at[r_p], lad.at[r], g_sem.at[0, 3], g_sem.at[1, 3], r_p, c)

    def stage(q):
        send_z(q).wait_recv()

        @pl.when(jnp.logical_not(own_ladder))
        def _():
            send_lx(q).start()

        send_y(q).wait_recv()

        @pl.when(q == OVER_Y)
        def _():
            send_dy(q).start()

        @pl.when(q != OVER_Y)
        def _():
            send_dz(q).start()

        @pl.when(q + AHEAD < NQ)
        def _():
            send_y(q + AHEAD).start()
            send_z(q + AHEAD).start()

            @pl.when(own_ladder)
            def _():
                send_lx(q + AHEAD).start()

    def on_step(q, step, act, *args):
        @pl.when(q == step)
        def _():
            act(*args)

    def go_row(q):
        send_row(q).start()

    with jax.named_scope("ph_stages"):
        stage(0)
        stage(1)

    @pl.loop(0, NQ)
    def _(q):
        on_step(q, 2, forward_ladder, 2)
        send_dz(q).wait_recv()

        @pl.when(q == NQ - 1)
        def _():
            lad_p.start()

        on_step(q, 0, go_lo, 0)

        def between():
            @pl.when(q + 2 < NQ)
            def _():
                stage(q + 2)

            on_step(q, 1, forward_ladder, 1)
            on_step(q, 1, go_row, 1)
            on_step(q, 2, forward_ladder, 3)
            on_step(q, 2, go_row, 2)
            on_step(q, 3, go_row, 3)

        particle_hole(q, between)

    n_pair = occ * occ
    pad = pl.ds(cols_dev - tail, LANES)
    for k in range(n_col):
        msg_p[k, :, pad] = jnp.zeros((n_pair, LANES), F32)
        msg_d[k, :, pad] = jnp.zeros((n_pair, LANES), F32)
        part[k, :, pad] = jnp.zeros((rows_dev, LANES), F32)

    @pl.loop(0, n_col)
    def _(k):
        for a in range(vir):
            msg_p[k, :, a * n_virt:(a + 1) * n_virt] = sp[:, k * vir + a, :]

    def p_send(off, width, n, k, p):
        at = pl.ds(off, width)
        return remote(msg_p.at[p, :, at], got_p.at[c, :, at], ps_sem.at[k, n], pr_sem.at[k, n], r, p)

    chunks = [(n * CHUNK, CHUNK) for n in range(n_full)] + [(n_full * CHUNK, LANES)]
    def go_p(first, last):
        for n, (off, width) in enumerate(chunks[first:last], first):
            for k, p in enumerate(col_peers):
                p_send(off, width, n, k, p).start()

    go_p(0, P_FIRST)
    own_p = pltpu.make_async_copy(msg_p.at[c], got_p.at[c], loc_sem.at[0])
    own_p.start()

    d_cut = n_full // 2 * CHUNK
    d_halves = ((0, d_cut), (d_cut, msg_d.shape[2] - d_cut))

    def d_send(w, k, p):
        at = pl.ds(*d_halves[w])
        return remote(msg_d.at[p, :, at], got_d.at[c, :, at], d_sem.at[0, w, k], d_sem.at[1, w, k], r, p)

    own_d = pltpu.make_async_copy(msg_d.at[c], got_d.at[c], loc_sem.at[1])

    def go_d(w):
        for k, p in enumerate(col_peers):
            d_send(w, k, p).start()

    def form_d():
        @pl.loop(0, n_col)
        def _(k):
            for a in range(vir):
                msg_d[k, :, a * n_virt:(a + 1) * n_virt] = sd[:, k * vir + a, :]

        go_d(0)
        own_d.start()

    ld_perm.wait()

    def permute(k, src):
        for off in range(0, cols_dev, CHUNK):
            width = min(CHUNK, cols_dev - off)
            block = jnp.dot(perm[...], src[:, off:off + width], preferred_element_type=F32)
            lad[k, :, off:off + width] = block.astype(BF16)

    permute(r, rows.at[r])
    lad_p.wait_recv()
    permute(r_p, lad.at[r_p])

    @pl.when(jnp.logical_not(direct))
    def _():
        for q in range(NQ):
            for w in range(2):
                send_ly(w, q).wait_recv()

    @pl.when(direct)
    def _():
        for w in range(2):
            recv_lx(w, 0).wait_recv()
        for q in range(1, NQ):
            for w in range(2):
                send_ly(w, q).wait_send()

    go_p(P_FIRST, P_AHEAD)

    @pl.loop(0, 2)
    def _(w):
        permute(2 * (1 - x) + w, lad.at[2 * (1 - x) + w])

    own_p.wait()

    for q in range(NQ):
        send_row(q).wait_recv()
    row_o.start()

    def h_send(off, width, n, w):
        at = pl.ds(off, width)
        return remote(part.at[2 * w + 1 - u, :, at], half.at[w, :, at], hs_sem.at[w, n], hr_sem.at[w, n], r_p, c)

    def x_pass(off, width, n):
        return remote(xsend.at[n, :, pl.ds(0, width)], xgot.at[n, :, pl.ds(0, width)], xs_sem.at[n], xr_sem.at[n], r_s, c)

    def across(off, width, n):
        at = pl.ds(off, width)
        with jax.named_scope("ph_wait_h"):
            for w in range(2):
                h_send(off, width, n, w).wait_recv()
        xsend[n, :, 0:width] = part[2 * (1 - x) + u, :, at] + half[1 - x, :, at]
        x_pass(off, width, n).start()

    def ladder(off, width, n, v_ref):
        at = pl.ds(off, width)
        with jax.named_scope("ph_dot"):
            t_all = lad[...].reshape(n_row * rows_dev, cols_dev)
            prod = jnp.dot(t_all, v_ref[:, 0:min(width, cols_dev - off) if width == LANES else width], preferred_element_type=F32)
            part[:, :, pl.ds(off, prod.shape[1])] = prod.reshape(n_row, rows_dev, prod.shape[1])
        with jax.named_scope("ph_wait_p"):
            for k, p in enumerate(col_peers):
                p_send(off, width, n, k, p).wait_recv()
        mine = pl.ds(pl.multiple_of(r * n_pair, n_pair), n_pair)
        for k in range(n_col):
            part[k, mine, at] += got_p[k, :, at]
        for w in range(2):
            h_send(off, width, n, w).start()

    def x_send(k, p):
        return remote(xpart, xgot_part.at[c], x_sem.at[0, k], x_sem.at[1, k], r, p)

    def form_x():
        row_p.wait_recv()
        row_o.wait_recv()
        ld_oovv.wait()
        for k in range(n_row):
            xpart[:, k * rows_dev:(k + 1) * rows_dev] = lax.dot_general(
                oovv[...], tcols[k], (((1,), (1,)), ((), ())), preferred_element_type=F32)
        for k, p in enumerate(col_peers):
            x_send(k, p).start()

    def m_send(k, p):
        return remote(m_mine.at[p], m_got.at[r], m_sem.at[0, k], m_sem.at[1, k], p, c)

    def form_m():
        for k, p in enumerate(col_peers):
            x_send(k, p).wait_recv()
        xgot_part[c] = xpart[...]
        x_sum = xgot_part[0] + xgot_part[1] + xgot_part[2] + xgot_part[3]
        ld_oooo.wait()
        hole = (oooo[pl.ds(pl.multiple_of(r * rows_dev, rows_dev), rows_dev), :].astype(F32) + 0.5 * x_sum)
        for k in range(n_row):
            m_mine[k] = hole[:, k * rows_dev:(k + 1) * rows_dev].astype(BF16)
        for k, p in enumerate(row_peers):
            m_send(k, p).start()
        m_got[r] = m_mine[r]

    @pl.loop(0, n_full)
    def _(n):
        off = pl.multiple_of(n * CHUNK, CHUNK)
        with jax.named_scope("ph_wait_v"):
            fetch(off, CHUNK, n % 2).wait()
        ladder(off, CHUNK, n, vbuf.at[n % 2])

        @pl.when(n + 2 < n_full)
        def _():
            fetch(pl.multiple_of((n + 2) * CHUNK, CHUNK), CHUNK, n % 2).start()

        @pl.when(n + P_AHEAD < n_full)
        def _():
            later = pl.multiple_of((n + P_AHEAD) * CHUNK, CHUNK)
            for k, p in enumerate(col_peers):
                p_send(later, CHUNK, n + P_AHEAD, k, p).start()

        @pl.when(n + P_AHEAD == n_full)
        def _():
            for k, p in enumerate(col_peers):
                p_send(n_full * CHUNK, LANES, n_full, k, p).start()

        @pl.when(n == 2)
        def _():
            with jax.named_scope("ph_form_x"):
                form_x()

        @pl.when(n == 6)
        def _():
            with jax.named_scope("ph_form_m"):
                form_m()

        @pl.when(n == D_FIRST)
        def _():
            with jax.named_scope("ph_form_d"):
                form_d()

        @pl.when(n == D_SECOND)
        def _():
            go_d(1)

        @pl.when(n == 0)
        def _():
            across(0, CHUNK, 0)

        @pl.when(n >= 2)
        def _():
            across(pl.multiple_of((n - 1) * CHUNK, CHUNK), CHUNK, n - 1)

    ladder(n_full * CHUNK, LANES, n_full, vlast)
    across((n_full - 1) * CHUNK, CHUNK, n_full - 1)
    across(n_full * CHUNK, LANES, n_full)

    with jax.named_scope("ph_fin_m"):
        for k, p in enumerate(row_peers):
            m_send(k, p).wait_recv()
    ld_den.wait()

    def hole_term(off, width):
        at = pl.ds(off, width)
        total = None
        for k in range(n_row):
            term = lax.dot_general(
                m_got[k], tcols[k, :, at], (((0,), (0,)), ((), ())), preferred_element_type=F32)
            total = term if total is None else total + term
        part[r_s, :, at] = total + oovv[:, at].astype(F32)
        part[r, :, pl.ds(off, width)] += half[x, :, at]

    def finish(off, width, n):
        at = pl.ds(off, width)
        own = part[r, :, at] + xgot[n, :, 0:width]
        for jh in range(n_col):
            v = own[jh * n_pair:(jh + 1) * n_pair] + got_d[jh, :, at]
            for i in range(occ):
                lo = i * n_occ + jh * occ
                turned[lo:lo + occ, 0:width] = v[i * occ:(i + 1) * occ]
        out[:, at] = (part[r_s, :, at] + turned[:, 0:width]) / t32[:, at]

    def full(n):
        return pl.multiple_of(n * CHUNK, CHUNK)

    @pl.loop(0, n_full)
    def _(n):
        hole_term(full(n), CHUNK)

    hole_term(n_full * CHUNK, tail)
    n_cut = d_cut // CHUNK

    def wait_d(w):
        with jax.named_scope("ph_fin_d"):
            for k, p in enumerate(col_peers):
                d_send(w, k, p).wait_recv()

    own_d.wait()
    wait_d(0)

    @pl.loop(0, n_full)
    def _(n):
        @pl.when(n == n_cut)
        def _():
            wait_d(1)

        with jax.named_scope("ph_fin_x"):
            x_pass(full(n), CHUNK, n).wait_recv()
        finish(full(n), CHUNK, n)

    x_pass(n_full * CHUNK, LANES, n_full).wait_recv()
    finish(n_full * CHUNK, tail, n_full)

    lad_p.wait_send()
    send_lo(0).wait_send()
    for q in range(NQ):
        send_y(q).wait_send()
        send_z(q).wait_send()
        send_dz(q).wait_send()
        send_row(q).wait_send()
        send_lx(q).wait_send()
    row_p.wait_send()
    row_o.wait_send()
    for k, p in enumerate(row_peers):
        m_send(k, p).wait_send()
    for k, p in enumerate(col_peers):
        x_send(k, p).wait_send()
        for w in range(2):
            d_send(w, k, p).wait_send()
    for n, (off, width) in enumerate(chunks):
        for k, p in enumerate(col_peers):
            p_send(off, width, n, k, p).wait_send()
        for w in range(2):
            h_send(off, width, n, w).wait_send()
        x_pass(off, width, n).wait_send()


def solution(mesh):
    n_row = mesh.shape["row"]
    n_col = mesh.shape["col"]
    amp_spec = P("row", "col")
    wide_spec = P(None, "col")

    def local_sweep(t_blk, d_blk, oovv_blk, vvvv_blk, oooo_full, wd_blk, wx_blk):
        rows_dev, cols_dev = t_blk.shape
        n_occ = math.isqrt(oooo_full.shape[0])
        n_virt = wd_blk.shape[0] // n_occ
        occ, vir = n_occ // n_row, n_virt // n_col
        n_pair = occ * occ
        n_chunk = cols_dev // CHUNK + 1
        wide = -(-cols_dev // LANES) * LANES
        kc, jb = wd_blk.shape
        perm = np.eye(rows_dev, dtype=BF16).reshape(occ, n_col, occ, rows_dev).transpose(1, 0, 2, 3).reshape(rows_dev, rows_dev)
        n_sq = n_occ * n_occ
        swap = np.eye(n_sq, dtype=BF16).reshape(n_occ, n_occ, n_sq).transpose(1, 0, 2).reshape(n_sq, n_sq)
        dma = pltpu.SemaphoreType.DMA
        vm = pltpu.VMEM
        hbm = pl.BlockSpec(memory_space=pl.ANY)
        block = (rows_dev, cols_dev)
        return pl.pallas_call(
            functools.partial(sweep_kernel, (n_occ, n_virt, n_row, n_col)),
            out_shape=pltpu.VMEM(block, F32),
            grid=(1,),
            in_specs=[hbm] * 4 + [pl.BlockSpec((cols_dev, LANES), lambda i: (0, cols_dev // LANES), pipeline_mode=pl.Buffered(1))] + [hbm] * 5,
            out_specs=pl.BlockSpec(memory_space=pltpu.VMEM),
            scratch_shapes=[
                vm(block, F32), vm((n_col,) + block, BF16), vm((n_row,) + block, BF16), vm((n_row,) + block, BF16),
                vm((kc, jb), BF16), vm((jb, kc), BF16), vm((jb, kc), BF16),
                vm((kc, n_virt), BF16), vm((n_virt, kc), BF16), vm((n_virt, jb), F32), vm((jb, n_virt), F32),
                vm((n_pair, n_virt, n_virt), F32), vm((n_pair, n_virt, n_virt), F32),
                vm((n_col, n_pair, wide), F32), vm((n_col, n_pair, wide), F32),
                vm((n_col, n_pair, wide), F32), vm((n_col, n_pair, wide), F32),
                vm((n_row, rows_dev, wide), F32), vm((2, rows_dev, wide), F32),
                vm((n_chunk, rows_dev, CHUNK), F32), vm((n_chunk, rows_dev, CHUNK), F32), vm((rows_dev, CHUNK), F32),
                vm((2, cols_dev, CHUNK), BF16), vm(block, BF16), vm(oooo_full.shape, BF16),
                vm((rows_dev, rows_dev), BF16), vm((n_sq, n_sq), BF16),
                vm((rows_dev, n_sq), F32), vm((n_col, rows_dev, n_sq), F32),
                vm((n_row, rows_dev, rows_dev), BF16), vm((n_row, rows_dev, rows_dev), BF16),
                dma((10,)), dma((2,)), dma((2,)), dma((3, NQ)), dma((3, NQ)), dma((4, NQ)), dma((4, NQ)), dma((2, 4)),
                dma((2, NQ)), dma((3, n_chunk)), dma((3, n_chunk)), dma((2, 2, 3)), dma((2, n_chunk)), dma((2, n_chunk)),
                dma((n_chunk,)), dma((n_chunk,)), dma((2, 3)), dma((2, 3)),
            ],
            compiler_params=pltpu.CompilerParams(
                collective_id=0, has_side_effects=True, vmem_limit_bytes=65536000),
        )(t_blk, d_blk, oovv_blk, vvvv_blk, vvvv_blk, oooo_full, wd_blk.T, wx_blk.T, jnp.asarray(perm), jnp.asarray(swap))

    return jax.shard_map(
        local_sweep, mesh=mesh,
        in_specs=(amp_spec, amp_spec, amp_spec, amp_spec, P(), wide_spec, wide_spec),
        out_specs=amp_spec, check_vma=False)
```

```python
import functools
import math

import jax
import jax.numpy as jnp
import numpy as np
from jax import lax
from jax.experimental import pallas as pl
from jax.experimental.pallas import tpu as pltpu
from jax.sharding import PartitionSpec as P

F32 = jnp.float32
BF16 = jnp.bfloat16
MESH = pl.DeviceIdType.MESH
CHUNK = 256
WIDE = 512
RING = 4
DEPTH = 4
LANES = 128
X_STEP, M_STEP = 6, 14
D_FIRST, D_SECOND = 9, 13
P_FIRST, P_AHEAD = 2, 6
AHEAD = 2
OVER_Y = 1
NQ = 4


def sweep_kernel(
    dims,
    t_hbm, den_hbm, oovv_hbm, vvvv_hbm, oooo_hbm, wd_hbm, wx_hbm, perm_hbm, swap_hbm,
    out,
    t32, rows, lad, tcols, wd, wdt, wxt, tr, ta, r3, r5, sd, sp, msg_d, msg_p, got_d, got_p,
    part, half, xsend, xgot, turned, vbuf, vlast, oovv, oooo, perm, swap, xpart, xgot_part, m_mine, m_got,
    in_sem, vb_sem, loc_sem, ts_sem, tr_sem, ls_sem, lr_sem, ly_sem, g_sem,
    rx_sem, ps_sem, pr_sem, d_sem, hs_sem, hr_sem, xs_sem, xr_sem, x_sem, m_sem,
):
    n_occ, n_virt, n_row, n_col = dims
    rows_dev, cols_dev = t32.shape
    occ = n_occ // n_row
    vir = n_virt // n_col
    qrows = rows_dev // NQ
    n_full = cols_dev // CHUNK
    tail = cols_dev - n_full * CHUNK
    r = lax.axis_index("row")
    c = lax.axis_index("col")
    x, u = r // 2, r % 2
    z, y = c // 2, c % 2
    c_y, c_z, c_d = 2 * z + 1 - y, 2 * (1 - z) + y, 2 * (1 - z) + 1 - y
    r_p, r_s, r_o = 2 * x + 1 - u, 2 * (1 - x) + u, 2 * (1 - x) + 1 - u
    col_peers = (c_y, c_z, c_d)
    row_peers = (r_p, r_s, r_o)

    def remote(src, dst, ssem, rsem, row, col):
        return pltpu.make_async_remote_copy(
            src_ref=src, dst_ref=dst, send_sem=ssem, recv_sem=rsem,
            device_id={"row": row, "col": col}, device_id_type=MESH)

    def load(src, dst, k):
        return pltpu.make_async_copy(src, dst, in_sem.at[k])

    ld_t = load(t_hbm, t32, 0)
    ld_wx = load(wx_hbm, wxt, 1)
    ld_wd = load(wd_hbm, wdt, 2)
    ld_oovv = load(oovv_hbm, oovv, 3)
    ld_oooo = load(oooo_hbm, oooo, 4)
    ld_perm = load(perm_hbm, perm, 5)
    ld_swap = load(swap_hbm, swap, 6)
    ld_den = load(den_hbm, t32, 7)
    for ld in (ld_t, ld_wx, ld_wd, ld_oovv, ld_oooo, ld_perm, ld_swap):
        ld.start()

    def fetch(off, width, slot):
        return pltpu.make_async_copy(vvvv_hbm.at[:, pl.ds(off, width)], vbuf.at[slot], vb_sem.at[slot])

    for s in range(DEPTH):
        fetch(s * CHUNK, CHUNK, s).start()

    ld_last = load(vvvv_hbm.at[:, pl.ds(n_full * CHUNK, tail)], vlast, 8)
    ld_last.start()
    barrier = pltpu.get_barrier_semaphore()
    for p in col_peers:
        pl.semaphore_signal(barrier, inc=1, device_id={"row": r, "col": p}, device_id_type=MESH)
    for p in row_peers:
        pl.semaphore_signal(barrier, inc=1, device_id={"row": p, "col": c}, device_id_type=MESH)
    pl.semaphore_wait(barrier, 6)

    def piece(ref, k, q):
        return ref.at[k, pl.ds(pl.multiple_of(q * qrows, qrows), qrows), :]

    def send_y(q):
        return remote(piece(rows, c, q), piece(rows, c, q), ts_sem.at[0], tr_sem.at[0, q], r, c_y)

    def send_z(q):
        return remote(piece(rows, c, q), piece(rows, c, q), ts_sem.at[1], tr_sem.at[1, q], r, c_z)

    def send_dz(q):
        return remote(piece(rows, c_y, q), piece(rows, c_y, q), ts_sem.at[2], tr_sem.at[2, q], r, c_z)

    def send_dy(q):
        return remote(piece(rows, c_z, q), piece(rows, c_z, q), ts_sem.at[2], tr_sem.at[2, q], r, c_y)

    blk_x = 2 * (1 - x) + y

    def send_lx(q):
        return remote(piece(rows, blk_x, q), piece(lad, r, q), ls_sem.at[0], lr_sem.at[u, q], blk_x, c)

    def recv_lx(w, q):
        k = 2 * (1 - x) + w
        return remote(piece(lad, k, q), piece(lad, k, q), ls_sem.at[0], lr_sem.at[w, q], blk_x, c)

    def send_ly(w, q):
        k = 2 * (1 - x) + w
        return remote(piece(lad, k, q), piece(lad, k, q), ls_sem.at[1 + w], ly_sem.at[w], r, c_y)

    def send_lo(q):
        k = 2 * (1 - x) + 1 - y
        return remote(piece(rows, k, q), piece(lad, r, q), ls_sem.at[3], ly_sem.at[u], k, c)

    def go_lo(q):
        send_lo(q).start()

    own_ladder = z == 1 - x
    direct = u == y

    ld_t.wait()
    for q in range(NQ):
        rows[c, pl.ds(q * qrows, qrows), :] = t32[pl.ds(q * qrows, qrows), :].astype(BF16)
        if q < AHEAD:
            send_y(q).start()
            send_z(q).start()

            @pl.when(own_ladder)
            def _():
                send_lx(q).start()

    ld_den.start()

    def send_row(q):
        return remote(piece(rows, c, q), piece(tcols, r, q), rx_sem.at[0], rx_sem.at[1], r_s, c)

    row_p = remote(rows.at[c], tcols.at[r], g_sem.at[0, 0], g_sem.at[1, 0], r_p, c)
    row_o = remote(tcols.at[r_s], tcols.at[r_s], g_sem.at[0, 1], g_sem.at[1, 1], r_p, c)
    row_p.start()
    send_row(0).start()
    tcols[r] = rows[c]

    with jax.named_scope("ph_turn_w"):
        ld_wd.wait()

        @pl.loop(0, wd.shape[0] // LANES)
        def _(m):
            at = pl.ds(pl.multiple_of(m * LANES, LANES), LANES)
            for b in range(0, wd.shape[1], LANES):
                w = min(LANES, wd.shape[1] - b)
                wd[at, b:b + w] = wdt[b:b + w, at].astype(F32).T.astype(BF16)

    def forward_ladder(q):
        @pl.when(direct)
        def _():
            for w in range(2):
                recv_lx(w, q).wait_recv()
                send_ly(w, q).start()

    ld_swap.wait()
    ld_wx.wait()

    def spread(i):
        lines = pl.ds(pl.multiple_of(i * n_occ, n_occ), n_occ)
        for ab in range(n_virt // n_occ):
            stack = []
            for t in range(n_occ):
                a = ab * n_occ + t
                lo = (a % vir) * n_virt
                stack.append(rows[a // vir, lines, lo:lo + n_virt])
            lines_k = jnp.dot(swap[...], jnp.concatenate(stack, axis=0), preferred_element_type=F32).astype(BF16)
            for k in range(n_occ):
                line = lines_k[k * n_occ:(k + 1) * n_occ]
                tr[k * n_virt + ab * n_occ:k * n_virt + (ab + 1) * n_occ, :] = line
                ta[ab * n_occ:(ab + 1) * n_occ, k * n_virt:(k + 1) * n_virt] = line

    def particle_hole(i, between):
        with jax.named_scope("ph_spread"):
            spread(i)
        with jax.named_scope("ph_r5"):
            r5[...] = jnp.dot(wxt[...], tr[...], preferred_element_type=F32)
            r3[...] = jnp.dot(ta[...], wd[...], preferred_element_type=F32)
        between()
        with jax.named_scope("ph_diff"):
            for j in range(occ):
                diff = r3[:, j * n_virt:(j + 1) * n_virt] - r5[j * n_virt:(j + 1) * n_virt, :]
                sd[i * occ + j] = diff
                sp[j * occ + i] = diff.T

    lad_p = remote(rows.at[r_p], lad.at[r], g_sem.at[0, 3], g_sem.at[1, 3], r_p, c)

    def stage(q):
        send_z(q).wait_recv()

        @pl.when(jnp.logical_not(own_ladder))
        def _():
            send_lx(q).start()

        send_y(q).wait_recv()

        @pl.when(q == OVER_Y)
        def _():
            send_dy(q).start()

        @pl.when(q != OVER_Y)
        def _():
            send_dz(q).start()

        @pl.when(q + AHEAD < NQ)
        def _():
            send_y(q + AHEAD).start()
            send_z(q + AHEAD).start()

            @pl.when(own_ladder)
            def _():
                send_lx(q + AHEAD).start()

    def on_step(q, step, act, *args):
        @pl.when(q == step)
        def _():
            act(*args)

    def go_row(q):
        send_row(q).start()

    with jax.named_scope("ph_stages"):
        stage(0)
        stage(1)

    @pl.loop(0, NQ)
    def _(q):
        on_step(q, 2, forward_ladder, 2)
        send_dz(q).wait_recv()

        @pl.when(q == NQ - 1)
        def _():
            lad_p.start()

        on_step(q, 0, go_lo, 0)

        def between():
            @pl.when(q + 2 < NQ)
            def _():
                stage(q + 2)

            on_step(q, 1, forward_ladder, 1)
            on_step(q, 1, go_row, 1)
            on_step(q, 2, forward_ladder, 3)
            on_step(q, 2, go_row, 2)
            on_step(q, 3, go_row, 3)

        particle_hole(q, between)

    n_pair = occ * occ
    pad = pl.ds(cols_dev - tail, LANES)
    for k in range(n_col):
        msg_p[k, :, pad] = jnp.zeros((n_pair, LANES), F32)
        msg_d[k, :, pad] = jnp.zeros((n_pair, LANES), F32)
        part[k, :, pad] = jnp.zeros((rows_dev, LANES), F32)

    @pl.loop(0, n_col)
    def _(k):
        for a in range(vir):
            msg_p[k, :, a * n_virt:(a + 1) * n_virt] = sp[:, k * vir + a, :]

    def p_send(off, width, n, k, p):
        at = pl.ds(off, width)
        return remote(msg_p.at[p, :, at], got_p.at[c, :, at], ps_sem.at[k], pr_sem.at[k, n], r, p)

    n_wide = cols_dev // WIDE
    chunks = [(n * WIDE, WIDE) for n in range(n_wide)] + [(n_wide * WIDE, LANES)]
    def go_p(first, last):
        for n, (off, width) in enumerate(chunks[first:last], first):
            for k, p in enumerate(col_peers):
                p_send(off, width, n, k, p).start()

    go_p(0, P_FIRST)
    own_p = pltpu.make_async_copy(msg_p.at[c], got_p.at[c], loc_sem.at[0])
    own_p.start()

    d_cut = n_full // 2 * CHUNK
    d_halves = ((0, d_cut), (d_cut, msg_d.shape[2] - d_cut))

    def d_send(w, k, p):
        at = pl.ds(*d_halves[w])
        return remote(msg_d.at[p, :, at], got_d.at[c, :, at], d_sem.at[0, k], d_sem.at[1 + w, k], r, p)

    own_d = pltpu.make_async_copy(msg_d.at[c], got_d.at[c], loc_sem.at[1])

    def go_d(w):
        for k, p in enumerate(col_peers):
            d_send(w, k, p).start()

    def form_d():
        @pl.loop(0, n_col)
        def _(k):
            for a in range(vir):
                msg_d[k, :, a * n_virt:(a + 1) * n_virt] = sd[:, k * vir + a, :]

        go_d(0)
        own_d.start()

    ld_perm.wait()

    def permute(k, src):
        for off in range(0, cols_dev, 4 * LANES):
            width = min(4 * LANES, cols_dev - off)
            block = jnp.dot(perm[...], src[:, off:off + width], preferred_element_type=F32)
            lad[k, :, off:off + width] = block.astype(BF16)

    permute(r, rows.at[r])
    lad_p.wait_recv()
    permute(r_p, lad.at[r_p])

    @pl.when(jnp.logical_not(direct))
    def _():
        for w in range(2):
            whole = lad.at[2 * (1 - x) + w]
            remote(whole, whole, ls_sem.at[1 + w], ly_sem.at[w], r, c_y).wait_recv()

    @pl.when(direct)
    def _():
        for w in range(2):
            recv_lx(w, 0).wait_recv()
        for w in range(2):
            rest = lad.at[2 * (1 - x) + w, pl.ds(qrows, rows_dev - qrows), :]
            remote(rest, rest, ls_sem.at[1 + w], ly_sem.at[w], r, c_y).wait_send()

    go_p(P_FIRST, P_AHEAD)

    @pl.loop(0, 2)
    def _(w):
        permute(2 * (1 - x) + w, lad.at[2 * (1 - x) + w])

    own_p.wait()

    remote(tcols.at[r_s], tcols.at[r_s], rx_sem.at[0], rx_sem.at[1], r_s, c).wait_recv()
    row_o.start()

    def h_send(off, width, n, w):
        at = pl.ds(off, width)
        return remote(part.at[2 * w + 1 - u, :, at], half.at[w, :, at], hs_sem.at[w], hr_sem.at[w, n % RING], r_p, c)

    def x_pass(off, width, n):
        return remote(xsend.at[n, :, pl.ds(0, width)], xgot.at[n, :, pl.ds(0, width)], xs_sem.at[0], xr_sem.at[n], r_s, c)

    def across(off, width, n):
        at = pl.ds(off, width)
        with jax.named_scope("ph_wait_h"):
            for w in range(2):
                h_send(off, width, n, w).wait_recv()
        xsend[n, :, 0:width] = part[2 * (1 - x) + u, :, at] + half[1 - x, :, at]
        x_pass(off, width, n).start()

    def ladder(off, width, n, v_ref, arrive):
        at = pl.ds(off, width)
        with jax.named_scope("ph_dot"):
            t_all = lad[...].reshape(n_row * rows_dev, cols_dev)
            prod = jnp.dot(t_all, v_ref[...], preferred_element_type=F32)
            part[:, :, pl.ds(off, prod.shape[1])] = prod.reshape(n_row, rows_dev, prod.shape[1])
        arrive()
        mine = pl.ds(pl.multiple_of(r * n_pair, n_pair), n_pair)
        for k in range(n_col):
            part[k, mine, at] += got_p[k, :, at]
        for w in range(2):
            h_send(off, width, n, w).start()

    def x_send(k, p):
        return remote(xpart, xgot_part.at[c], x_sem.at[0, k], x_sem.at[1, k], r, p)

    def form_x():
        row_p.wait_recv()
        row_o.wait_recv()
        ld_oovv.wait()
        for k in range(n_row):
            xpart[:, k * rows_dev:(k + 1) * rows_dev] = lax.dot_general(
                oovv[...], tcols[k], (((1,), (1,)), ((), ())), preferred_element_type=F32)
        for k, p in enumerate(col_peers):
            x_send(k, p).start()

    def m_send(k, p):
        return remote(m_mine.at[p], m_got.at[r], m_sem.at[0, k], m_sem.at[1, k], p, c)

    def form_m():
        for k, p in enumerate(col_peers):
            x_send(k, p).wait_recv()
        xgot_part[c] = xpart[...]
        x_sum = xgot_part[0] + xgot_part[1] + xgot_part[2] + xgot_part[3]
        ld_oooo.wait()
        hole = (oooo[pl.ds(pl.multiple_of(r * rows_dev, rows_dev), rows_dev), :].astype(F32) + 0.5 * x_sum)
        for k in range(n_row):
            m_mine[k] = hole[:, k * rows_dev:(k + 1) * rows_dev].astype(BF16)
        for k, p in enumerate(row_peers):
            m_send(k, p).start()
        m_got[r] = m_mine[r]

    per = WIDE // CHUNK

    @pl.loop(0, n_full)
    def _(n):
        off = pl.multiple_of(n * CHUNK, CHUNK)
        with jax.named_scope("ph_wait_v"):
            fetch(off, CHUNK, n % DEPTH).wait()
        m = n // per
        p_off = pl.multiple_of(m * WIDE, WIDE)

        def arrive():
            @pl.when(n % per == 0)
            def _():
                for k, p in enumerate(col_peers):
                    p_send(p_off, WIDE, m, k, p).wait_recv()

        ladder(off, CHUNK, n, vbuf.at[n % DEPTH], arrive)

        @pl.when(n + DEPTH < n_full)
        def _():
            fetch(pl.multiple_of((n + DEPTH) * CHUNK, CHUNK), CHUNK, n % DEPTH).start()

        @pl.when(jnp.logical_and(n % per == 0, m + P_AHEAD < n_wide))
        def _():
            later = pl.multiple_of((m + P_AHEAD) * WIDE, WIDE)
            for k, p in enumerate(col_peers):
                p_send(later, WIDE, m + P_AHEAD, k, p).start()

        @pl.when(n == (n_wide - P_AHEAD) * per)
        def _():
            for k, p in enumerate(col_peers):
                p_send(n_wide * WIDE, LANES, n_wide, k, p).start()

        @pl.when(n == X_STEP)
        def _():
            with jax.named_scope("ph_form_x"):
                form_x()

        @pl.when(n == M_STEP)
        def _():
            with jax.named_scope("ph_form_m"):
                form_m()

        @pl.when(n == D_FIRST)
        def _():
            with jax.named_scope("ph_form_d"):
                form_d()

        @pl.when(n == D_SECOND)
        def _():
            go_d(1)

        @pl.when(n == 0)
        def _():
            across(0, CHUNK, 0)

        @pl.when(n >= 2)
        def _():
            across(pl.multiple_of((n - 1) * CHUNK, CHUNK), CHUNK, n - 1)

    ld_last.wait()
    def arrive_last():
        for k, p in enumerate(col_peers):
            p_send(n_wide * WIDE, LANES, n_wide, k, p).wait_recv()

    ladder(n_full * CHUNK, LANES, n_full, vlast, arrive_last)
    across((n_full - 1) * CHUNK, CHUNK, n_full - 1)
    across(n_full * CHUNK, LANES, n_full)

    with jax.named_scope("ph_fin_m"):
        for k, p in enumerate(row_peers):
            m_send(k, p).wait_recv()
    ld_den.wait()

    def hole_term(off, width):
        at = pl.ds(off, width)
        total = None
        for k in range(n_row):
            term = lax.dot_general(
                m_got[k], tcols[k, :, at], (((0,), (0,)), ((), ())), preferred_element_type=F32)
            total = term if total is None else total + term
        part[r_s, :, at] = total + oovv[:, at].astype(F32)
        part[r, :, pl.ds(off, width)] += half[x, :, at]

    def finish(off, width, n):
        at = pl.ds(off, width)
        own = part[r, :, at] + xgot[n, :, 0:width]
        for jh in range(n_col):
            v = own[jh * n_pair:(jh + 1) * n_pair] + got_d[jh, :, at]
            for i in range(occ):
                lo = i * n_occ + jh * occ
                turned[lo:lo + occ, 0:width] = v[i * occ:(i + 1) * occ]
        out[:, at] = (part[r_s, :, at] + turned[:, 0:width]) / t32[:, at]

    def full(n):
        return pl.multiple_of(n * CHUNK, CHUNK)

    @pl.loop(0, n_full)
    def _(n):
        hole_term(full(n), CHUNK)

    hole_term(n_full * CHUNK, tail)
    n_cut = d_cut // CHUNK

    def wait_d(w):
        with jax.named_scope("ph_fin_d"):
            for k, p in enumerate(col_peers):
                d_send(w, k, p).wait_recv()

    lad_p.wait_send()
    send_lo(0).wait_send()
    row_p.wait_send()
    row_o.wait_send()
    own = rows.at[c]
    for k in range(3):
        remote(own, own, ts_sem.at[k], tr_sem.at[0, 0], r, c_y).wait_send()
    remote(own, own, ls_sem.at[0], tr_sem.at[0, 0], r, c_y).wait_send()
    remote(own, own, rx_sem.at[0], rx_sem.at[1], r_s, c).wait_send()
    for k, p in enumerate(row_peers):
        m_send(k, p).wait_send()
    for k, p in enumerate(col_peers):
        x_send(k, p).wait_send()
        remote(msg_p.at[p], got_p.at[c], ps_sem.at[k], pr_sem.at[k, 0], r, p).wait_send()
    for w in range(2):
        remote(part.at[2 * w + 1 - u], half.at[w], hs_sem.at[w], hr_sem.at[w, 0], r_p, c).wait_send()

    own_d.wait()
    wait_d(0)

    @pl.loop(0, n_full)
    def _(n):
        @pl.when(n == n_cut)
        def _():
            wait_d(1)

        with jax.named_scope("ph_fin_x"):
            x_pass(full(n), CHUNK, n).wait_recv()
        finish(full(n), CHUNK, n)

    x_pass(n_full * CHUNK, LANES, n_full).wait_recv()
    finish(n_full * CHUNK, tail, n_full)
    for k, p in enumerate(col_peers):
        remote(msg_d.at[p], got_d.at[c], d_sem.at[0, k], d_sem.at[1, k], r, p).wait_send()
    remote(part.at[r], half.at[0], xs_sem.at[0], xr_sem.at[0], r_s, c).wait_send()


def solution(mesh):
    n_row = mesh.shape["row"]
    n_col = mesh.shape["col"]
    amp_spec = P("row", "col")
    wide_spec = P(None, "col")

    def local_sweep(t_blk, d_blk, oovv_blk, vvvv_blk, oooo_full, wd_blk, wx_blk):
        rows_dev, cols_dev = t_blk.shape
        n_occ = math.isqrt(oooo_full.shape[0])
        n_virt = wd_blk.shape[0] // n_occ
        occ, vir = n_occ // n_row, n_virt // n_col
        n_pair = occ * occ
        n_chunk = cols_dev // CHUNK + 1
        wide = -(-cols_dev // LANES) * LANES
        kc, jb = wd_blk.shape
        perm = np.eye(rows_dev, dtype=BF16).reshape(occ, n_col, occ, rows_dev).transpose(1, 0, 2, 3).reshape(rows_dev, rows_dev)
        n_sq = n_occ * n_occ
        swap = np.eye(n_sq, dtype=BF16).reshape(n_occ, n_occ, n_sq).transpose(1, 0, 2).reshape(n_sq, n_sq)
        dma = pltpu.SemaphoreType.DMA
        vm = pltpu.VMEM
        hbm = pl.BlockSpec(memory_space=pl.ANY)
        block = (rows_dev, cols_dev)
        return pl.pallas_call(
            functools.partial(sweep_kernel, (n_occ, n_virt, n_row, n_col)),
            out_shape=pltpu.VMEM(block, F32),
            in_specs=[hbm] * 9,
            out_specs=pl.BlockSpec(memory_space=pltpu.VMEM),
            scratch_shapes=[
                vm(block, F32), vm((n_col,) + block, BF16), vm((n_row,) + block, BF16), vm((n_row,) + block, BF16),
                vm((kc, jb), BF16), vm((jb, kc), BF16), vm((jb, kc), BF16),
                vm((kc, n_virt), BF16), vm((n_virt, kc), BF16), vm((n_virt, jb), F32), vm((jb, n_virt), F32),
                vm((n_pair, n_virt, n_virt), F32), vm((n_pair, n_virt, n_virt), F32),
                vm((n_col, n_pair, wide), F32), vm((n_col, n_pair, wide), F32),
                vm((n_col, n_pair, wide), F32), vm((n_col, n_pair, wide), F32),
                vm((n_row, rows_dev, wide), F32), vm((2, rows_dev, wide), F32),
                vm((n_chunk, rows_dev, CHUNK), F32), vm((n_chunk, rows_dev, CHUNK), F32), vm((rows_dev, CHUNK), F32),
                vm((DEPTH, cols_dev, CHUNK), BF16), vm((cols_dev, cols_dev % CHUNK), BF16), vm(block, BF16), vm(oooo_full.shape, BF16),
                vm((rows_dev, rows_dev), BF16), vm((n_sq, n_sq), BF16),
                vm((rows_dev, n_sq), F32), vm((n_col, rows_dev, n_sq), F32),
                vm((n_row, rows_dev, rows_dev), BF16), vm((n_row, rows_dev, rows_dev), BF16),
                dma((9,)), dma((DEPTH,)), dma((2,)), dma((3,)), dma((3, NQ)), dma((4,)), dma((2, NQ)), dma((2,)), dma((2, 4)),
                dma((2,)), dma((3,)), dma((3, cols_dev // WIDE + 1)), dma((3, 3)), dma((2,)), dma((2, RING)),
                dma((1,)), dma((n_chunk,)), dma((2, 3)), dma((2, 3)),
            ],
            compiler_params=pltpu.CompilerParams(
                collective_id=0, has_side_effects=True, vmem_limit_bytes=65536000),
        )(t_blk, d_blk, oovv_blk, vvvv_blk, oooo_full, wd_blk.T, wx_blk.T, jnp.asarray(perm), jnp.asarray(swap))

    return jax.shard_map(
        local_sweep, mesh=mesh,
        in_specs=(amp_spec, amp_spec, amp_spec, amp_spec, P(), wide_spec, wide_spec),
        out_specs=amp_spec, check_vma=False)
```

```python
import functools
import math

import jax
import jax.numpy as jnp
import numpy as np
from jax import lax
from jax.experimental import pallas as pl
from jax.experimental.pallas import tpu as pltpu
from jax.sharding import PartitionSpec as P

F32 = jnp.float32
BF16 = jnp.bfloat16
MESH = pl.DeviceIdType.MESH
CHUNK = 256
WIDE = 512
RING = 4
DEPTH = 4
LANES = 128
ROW_STEP, X_STEP, M_STEP = 3, 6, 14
D_FIRST, D_SECOND = 9, 13
P_FIRST, P_AHEAD = 2, 6
AHEAD = 2
OVER_Y = 1
NQ = 4


def sweep_kernel(
    dims,
    t_hbm, den_hbm, oovv_hbm, vvvv_hbm, oooo_hbm, wd_hbm, wx_hbm, perm_hbm, swap_hbm,
    out,
    t32, rows, lad, tcols, wd, wdt, wxt, tr, ta, r3, r5, sd, sp, msg_d, msg_p, got_d, got_p,
    part, half, xsend, xgot, turned, vbuf, vlast, oovv, oooo, perm, swap, xpart, xgot_part, m_mine, m_got,
    in_sem, vb_sem, loc_sem, ts_sem, tr_sem, ls_sem, lr_sem, ly_sem, g_sem,
    rx_sem, ps_sem, pr_sem, d_sem, hs_sem, hr_sem, xs_sem, xr_sem, x_sem, m_sem,
):
    n_occ, n_virt, n_row, n_col = dims
    rows_dev, cols_dev = t32.shape
    occ = n_occ // n_row
    vir = n_virt // n_col
    qrows = rows_dev // NQ
    n_full = cols_dev // CHUNK
    tail = cols_dev - n_full * CHUNK
    r = lax.axis_index("row")
    c = lax.axis_index("col")
    x, u = r // 2, r % 2
    z, y = c // 2, c % 2
    c_y, c_z, c_d = 2 * z + 1 - y, 2 * (1 - z) + y, 2 * (1 - z) + 1 - y
    r_p, r_s, r_o = 2 * x + 1 - u, 2 * (1 - x) + u, 2 * (1 - x) + 1 - u
    col_peers = (c_y, c_z, c_d)
    row_peers = (r_p, r_s, r_o)

    def remote(src, dst, ssem, rsem, row, col):
        return pltpu.make_async_remote_copy(
            src_ref=src, dst_ref=dst, send_sem=ssem, recv_sem=rsem,
            device_id={"row": row, "col": col}, device_id_type=MESH)

    def load(src, dst, k):
        return pltpu.make_async_copy(src, dst, in_sem.at[k])

    def ld_t(q):
        at = pl.ds(q * qrows, qrows)
        return load(t_hbm.at[at, :], t32.at[at, :], 9 + q)

    for q in range(NQ):
        ld_t(q).start()
    ld_wx = load(wx_hbm, wxt, 1)
    ld_wd = load(wd_hbm, wdt, 2)
    ld_oovv = load(oovv_hbm, oovv, 3)
    ld_oooo = load(oooo_hbm, oooo, 4)
    ld_perm = load(perm_hbm, perm, 5)
    ld_swap = load(swap_hbm, swap, 6)
    ld_den = load(den_hbm, t32, 7)

    def fetch(off, width, slot):
        return pltpu.make_async_copy(vvvv_hbm.at[:, pl.ds(off, width)], vbuf.at[slot], vb_sem.at[slot])

    barrier = pltpu.get_barrier_semaphore()
    for p in col_peers:
        pl.semaphore_signal(barrier, inc=1, device_id={"row": r, "col": p}, device_id_type=MESH)
    for p in row_peers:
        pl.semaphore_signal(barrier, inc=1, device_id={"row": p, "col": c}, device_id_type=MESH)
    pl.semaphore_wait(barrier, 6)

    def piece(ref, k, q):
        return ref.at[k, pl.ds(pl.multiple_of(q * qrows, qrows), qrows), :]

    def send_y(q):
        return remote(piece(rows, c, q), piece(rows, c, q), ts_sem.at[0], tr_sem.at[0, q], r, c_y)

    def send_z(q):
        return remote(piece(rows, c, q), piece(rows, c, q), ts_sem.at[1], tr_sem.at[1, q], r, c_z)

    def send_dz(q):
        return remote(piece(rows, c_y, q), piece(rows, c_y, q), ts_sem.at[2], tr_sem.at[2, q], r, c_z)

    def send_dy(q):
        return remote(piece(rows, c_z, q), piece(rows, c_z, q), ts_sem.at[2], tr_sem.at[2, q], r, c_y)

    blk_x = 2 * (1 - x) + y

    def send_lx(q):
        return remote(piece(rows, blk_x, q), piece(lad, r, q), ls_sem.at[0], lr_sem.at[u, q], blk_x, c)

    def recv_lx(w, q):
        k = 2 * (1 - x) + w
        return remote(piece(lad, k, q), piece(lad, k, q), ls_sem.at[0], lr_sem.at[w, q], blk_x, c)

    def send_ly(w, q):
        k = 2 * (1 - x) + w
        return remote(piece(lad, k, q), piece(lad, k, q), ls_sem.at[1 + w], ly_sem.at[w], r, c_y)

    def send_lo(q):
        k = 2 * (1 - x) + 1 - y
        return remote(piece(rows, k, q), piece(lad, r, q), ls_sem.at[3], ly_sem.at[u], k, c)

    def go_lo(q):
        send_lo(q).start()

    own_ladder = z == 1 - x
    direct = u == y

    for q in range(NQ):
        ld_t(q).wait()
        rows[c, pl.ds(q * qrows, qrows), :] = t32[pl.ds(q * qrows, qrows), :].astype(BF16)
        if q < AHEAD:
            send_y(q).start()
            send_z(q).start()

            @pl.when(own_ladder)
            def _():
                send_lx(q).start()

    for ld in (ld_wd, ld_wx, ld_swap, ld_perm, ld_oovv, ld_oooo):
        ld.start()
    ld_den.start()
    for s in range(DEPTH):
        fetch(s * CHUNK, CHUNK, s).start()

    ld_last = load(vvvv_hbm.at[:, pl.ds(n_full * CHUNK, tail)], vlast, 8)
    ld_last.start()

    def send_row(q):
        return remote(piece(rows, c, q), piece(tcols, r, q), rx_sem.at[0], rx_sem.at[1], r_s, c)

    row_p = remote(rows.at[c], tcols.at[r], g_sem.at[0, 0], g_sem.at[1, 0], r_p, c)
    row_o = remote(tcols.at[r_s], tcols.at[r_s], g_sem.at[0, 1], g_sem.at[1, 1], r_p, c)
    row_p.start()
    send_row(0).start()
    tcols[r] = rows[c]

    with jax.named_scope("ph_turn_w"):
        ld_wd.wait()

        @pl.loop(0, wd.shape[0] // LANES)
        def _(m):
            at = pl.ds(pl.multiple_of(m * LANES, LANES), LANES)
            for b in range(0, wd.shape[1], LANES):
                w = min(LANES, wd.shape[1] - b)
                wd[at, b:b + w] = wdt[b:b + w, at].astype(F32).T.astype(BF16)

    def forward_ladder(q):
        @pl.when(direct)
        def _():
            for w in range(2):
                recv_lx(w, q).wait_recv()
                send_ly(w, q).start()

    ld_swap.wait()
    ld_wx.wait()

    def spread(i):
        lines = pl.ds(pl.multiple_of(i * n_occ, n_occ), n_occ)
        for ab in range(n_virt // n_occ):
            stack = []
            for t in range(n_occ):
                a = ab * n_occ + t
                lo = (a % vir) * n_virt
                stack.append(rows[a // vir, lines, lo:lo + n_virt])
            lines_k = jnp.dot(swap[...], jnp.concatenate(stack, axis=0), preferred_element_type=F32).astype(BF16)
            for k in range(n_occ):
                line = lines_k[k * n_occ:(k + 1) * n_occ]
                tr[k * n_virt + ab * n_occ:k * n_virt + (ab + 1) * n_occ, :] = line
                ta[ab * n_occ:(ab + 1) * n_occ, k * n_virt:(k + 1) * n_virt] = line

    def particle_hole(i, between):
        with jax.named_scope("ph_spread"):
            spread(i)
        with jax.named_scope("ph_r5"):
            r5[...] = jnp.dot(wxt[...], tr[...], preferred_element_type=F32)
            r3[...] = jnp.dot(ta[...], wd[...], preferred_element_type=F32)
        between()
        with jax.named_scope("ph_diff"):
            for j in range(occ):
                diff = r3[:, j * n_virt:(j + 1) * n_virt] - r5[j * n_virt:(j + 1) * n_virt, :]
                sd[i * occ + j] = diff
                sp[j * occ + i] = diff.T

    lad_p = remote(rows.at[r_p], lad.at[r], g_sem.at[0, 3], g_sem.at[1, 3], r_p, c)

    def stage(q):
        send_z(q).wait_recv()

        @pl.when(jnp.logical_not(own_ladder))
        def _():
            send_lx(q).start()

        send_y(q).wait_recv()

        @pl.when(q == OVER_Y)
        def _():
            send_dy(q).start()

        @pl.when(q != OVER_Y)
        def _():
            send_dz(q).start()

        @pl.when(q + AHEAD < NQ)
        def _():
            send_y(q + AHEAD).start()
            send_z(q + AHEAD).start()

            @pl.when(own_ladder)
            def _():
                send_lx(q + AHEAD).start()

    def on_step(q, step, act, *args):
        @pl.when(q == step)
        def _():
            act(*args)

    def go_row(q):
        send_row(q).start()

    with jax.named_scope("ph_stages"):
        stage(0)
        stage(1)

    @pl.loop(0, NQ)
    def _(q):
        on_step(q, 2, forward_ladder, 2)
        send_dz(q).wait_recv()

        @pl.when(q == NQ - 1)
        def _():
            lad_p.start()

        on_step(q, 0, go_lo, 0)

        def between():
            @pl.when(q + 2 < NQ)
            def _():
                stage(q + 2)

            on_step(q, 0, forward_ladder, 1)
            on_step(q, 1, go_row, 1)
            on_step(q, 2, forward_ladder, 3)
            on_step(q, 2, go_row, 2)
            on_step(q, 3, go_row, 3)

        particle_hole(q, between)

    n_pair = occ * occ
    pad = pl.ds(cols_dev - tail, LANES)
    for k in range(n_col):
        msg_p[k, :, pad] = jnp.zeros((n_pair, LANES), F32)
        msg_d[k, :, pad] = jnp.zeros((n_pair, LANES), F32)
        part[k, :, pad] = jnp.zeros((rows_dev, LANES), F32)

    @pl.loop(0, n_col)
    def _(k):
        for a in range(vir):
            msg_p[k, :, a * n_virt:(a + 1) * n_virt] = sp[:, k * vir + a, :]

    def p_send(off, width, n, k, p):
        at = pl.ds(off, width)
        return remote(msg_p.at[p, :, at], got_p.at[c, :, at], ps_sem.at[k], pr_sem.at[k, n], r, p)

    n_wide = cols_dev // WIDE
    chunks = [(n * WIDE, WIDE) for n in range(n_wide)] + [(n_wide * WIDE, LANES)]
    def go_p(first, last):
        for n, (off, width) in enumerate(chunks[first:last], first):
            for k, p in enumerate(col_peers):
                p_send(off, width, n, k, p).start()

    go_p(0, P_FIRST)
    own_p = pltpu.make_async_copy(msg_p.at[c], got_p.at[c], loc_sem.at[0])
    own_p.start()

    d_cut = n_full // 2 * CHUNK
    d_halves = ((0, d_cut), (d_cut, msg_d.shape[2] - d_cut))

    def d_send(w, k, p):
        at = pl.ds(*d_halves[w])
        return remote(msg_d.at[p, :, at], got_d.at[c, :, at], d_sem.at[0, k], d_sem.at[1 + w, k], r, p)

    own_d = pltpu.make_async_copy(msg_d.at[c], got_d.at[c], loc_sem.at[1])

    def go_d(w):
        for k, p in enumerate(col_peers):
            d_send(w, k, p).start()

    def form_d():
        @pl.loop(0, n_col)
        def _(k):
            for a in range(vir):
                msg_d[k, :, a * n_virt:(a + 1) * n_virt] = sd[:, k * vir + a, :]

        go_d(0)
        own_d.start()

    ld_perm.wait()

    def permute(k, src):
        for off in range(0, cols_dev, 4 * LANES):
            width = min(4 * LANES, cols_dev - off)
            block = jnp.dot(perm[...], src[:, off:off + width], preferred_element_type=F32)
            lad[k, :, off:off + width] = block.astype(BF16)

    permute(r, rows.at[r])
    lad_p.wait_recv()
    permute(r_p, lad.at[r_p])

    @pl.when(jnp.logical_not(direct))
    def _():
        for w in range(2):
            whole = lad.at[2 * (1 - x) + w]
            remote(whole, whole, ls_sem.at[1 + w], ly_sem.at[w], r, c_y).wait_recv()

    @pl.when(direct)
    def _():
        for w in range(2):
            recv_lx(w, 0).wait_recv()
        for w in range(2):
            rest = lad.at[2 * (1 - x) + w, pl.ds(qrows, rows_dev - qrows), :]
            remote(rest, rest, ls_sem.at[1 + w], ly_sem.at[w], r, c_y).wait_send()

    go_p(P_FIRST, P_AHEAD)

    @pl.loop(0, 2)
    def _(w):
        permute(2 * (1 - x) + w, lad.at[2 * (1 - x) + w])

    own_p.wait()


    def h_send(off, width, n, w):
        at = pl.ds(off, width)
        return remote(part.at[2 * w + 1 - u, :, at], half.at[w, :, at], hs_sem.at[w], hr_sem.at[w, n % RING], r_p, c)

    def x_pass(off, width, n):
        return remote(xsend.at[n, :, pl.ds(0, width)], xgot.at[n, :, pl.ds(0, width)], xs_sem.at[0], xr_sem.at[n], r_s, c)

    def across(off, width, n):
        at = pl.ds(off, width)
        with jax.named_scope("ph_wait_h"):
            for w in range(2):
                h_send(off, width, n, w).wait_recv()
        xsend[n, :, 0:width] = part[2 * (1 - x) + u, :, at] + half[1 - x, :, at]
        x_pass(off, width, n).start()

    def ladder(off, width, n, v_ref, arrive):
        at = pl.ds(off, width)
        with jax.named_scope("ph_dot"):
            t_all = lad[...].reshape(n_row * rows_dev, cols_dev)
            prod = jnp.dot(t_all, v_ref[...], preferred_element_type=F32)
            part[:, :, pl.ds(off, prod.shape[1])] = prod.reshape(n_row, rows_dev, prod.shape[1])
        arrive()
        mine = pl.ds(pl.multiple_of(r * n_pair, n_pair), n_pair)
        for k in range(n_col):
            part[k, mine, at] += got_p[k, :, at]
        for w in range(2):
            h_send(off, width, n, w).start()

    def x_send(k, p):
        return remote(xpart, xgot_part.at[c], x_sem.at[0, k], x_sem.at[1, k], r, p)

    def form_x():
        row_p.wait_recv()
        row_o.wait_recv()
        ld_oovv.wait()
        for k in range(n_row):
            xpart[:, k * rows_dev:(k + 1) * rows_dev] = lax.dot_general(
                oovv[...], tcols[k], (((1,), (1,)), ((), ())), preferred_element_type=F32)
        for k, p in enumerate(col_peers):
            x_send(k, p).start()

    def m_send(k, p):
        return remote(m_mine.at[p], m_got.at[r], m_sem.at[0, k], m_sem.at[1, k], p, c)

    def form_m():
        for k, p in enumerate(col_peers):
            x_send(k, p).wait_recv()
        xgot_part[c] = xpart[...]
        x_sum = xgot_part[0] + xgot_part[1] + xgot_part[2] + xgot_part[3]
        ld_oooo.wait()
        hole = (oooo[pl.ds(pl.multiple_of(r * rows_dev, rows_dev), rows_dev), :].astype(F32) + 0.5 * x_sum)
        for k in range(n_row):
            m_mine[k] = hole[:, k * rows_dev:(k + 1) * rows_dev].astype(BF16)
        for k, p in enumerate(row_peers):
            m_send(k, p).start()
        m_got[r] = m_mine[r]

    per = WIDE // CHUNK

    @pl.loop(0, n_full)
    def _(n):
        off = pl.multiple_of(n * CHUNK, CHUNK)
        with jax.named_scope("ph_wait_v"):
            fetch(off, CHUNK, n % DEPTH).wait()
        m = n // per
        p_off = pl.multiple_of(m * WIDE, WIDE)

        def arrive():
            @pl.when(n % per == 0)
            def _():
                for k, p in enumerate(col_peers):
                    p_send(p_off, WIDE, m, k, p).wait_recv()

        ladder(off, CHUNK, n, vbuf.at[n % DEPTH], arrive)

        @pl.when(n + DEPTH < n_full)
        def _():
            fetch(pl.multiple_of((n + DEPTH) * CHUNK, CHUNK), CHUNK, n % DEPTH).start()

        @pl.when(jnp.logical_and(n % per == 0, m + P_AHEAD < n_wide))
        def _():
            later = pl.multiple_of((m + P_AHEAD) * WIDE, WIDE)
            for k, p in enumerate(col_peers):
                p_send(later, WIDE, m + P_AHEAD, k, p).start()

        @pl.when(n == (n_wide - P_AHEAD) * per)
        def _():
            for k, p in enumerate(col_peers):
                p_send(n_wide * WIDE, LANES, n_wide, k, p).start()

        @pl.when(n == ROW_STEP)
        def _():
            remote(tcols.at[r_s], tcols.at[r_s], rx_sem.at[0], rx_sem.at[1], r_s, c).wait_recv()
            row_o.start()

        @pl.when(n == X_STEP)
        def _():
            with jax.named_scope("ph_form_x"):
                form_x()

        @pl.when(n == M_STEP)
        def _():
            with jax.named_scope("ph_form_m"):
                form_m()

        @pl.when(n == D_FIRST)
        def _():
            with jax.named_scope("ph_form_d"):
                form_d()

        @pl.when(n == D_SECOND)
        def _():
            go_d(1)

        @pl.when(n == 0)
        def _():
            across(0, CHUNK, 0)

        @pl.when(n >= 2)
        def _():
            across(pl.multiple_of((n - 1) * CHUNK, CHUNK), CHUNK, n - 1)

    ld_last.wait()
    def arrive_last():
        for k, p in enumerate(col_peers):
            p_send(n_wide * WIDE, LANES, n_wide, k, p).wait_recv()

    ladder(n_full * CHUNK, LANES, n_full, vlast, arrive_last)
    across((n_full - 1) * CHUNK, CHUNK, n_full - 1)
    across(n_full * CHUNK, LANES, n_full)

    with jax.named_scope("ph_fin_m"):
        for k, p in enumerate(row_peers):
            m_send(k, p).wait_recv()
    ld_den.wait()

    def hole_term(off, width):
        at = pl.ds(off, width)
        total = None
        for k in range(n_row):
            term = lax.dot_general(
                m_got[k], tcols[k, :, at], (((0,), (0,)), ((), ())), preferred_element_type=F32)
            total = term if total is None else total + term
        part[r_s, :, at] = total + oovv[:, at].astype(F32)
        part[r, :, pl.ds(off, width)] += half[x, :, at]

    def finish(off, width, n):
        at = pl.ds(off, width)
        own = part[r, :, at] + xgot[n, :, 0:width]
        for jh in range(n_col):
            v = own[jh * n_pair:(jh + 1) * n_pair] + got_d[jh, :, at]
            for i in range(occ):
                lo = i * n_occ + jh * occ
                turned[lo:lo + occ, 0:width] = v[i * occ:(i + 1) * occ]
        out[:, at] = (part[r_s, :, at] + turned[:, 0:width]) / t32[:, at]

    def full(n):
        return pl.multiple_of(n * CHUNK, CHUNK)

    @pl.loop(0, n_full)
    def _(n):
        hole_term(full(n), CHUNK)

    hole_term(n_full * CHUNK, tail)
    n_cut = d_cut // CHUNK

    def wait_d(w):
        with jax.named_scope("ph_fin_d"):
            for k, p in enumerate(col_peers):
                d_send(w, k, p).wait_recv()

    lad_p.wait_send()
    send_lo(0).wait_send()
    row_p.wait_send()
    row_o.wait_send()
    own = rows.at[c]
    for k in range(3):
        remote(own, own, ts_sem.at[k], tr_sem.at[0, 0], r, c_y).wait_send()
    remote(own, own, ls_sem.at[0], tr_sem.at[0, 0], r, c_y).wait_send()
    remote(own, own, rx_sem.at[0], rx_sem.at[1], r_s, c).wait_send()
    for k, p in enumerate(row_peers):
        m_send(k, p).wait_send()
    for k, p in enumerate(col_peers):
        x_send(k, p).wait_send()
        remote(msg_p.at[p], got_p.at[c], ps_sem.at[k], pr_sem.at[k, 0], r, p).wait_send()
    for w in range(2):
        remote(part.at[2 * w + 1 - u], half.at[w], hs_sem.at[w], hr_sem.at[w, 0], r_p, c).wait_send()

    own_d.wait()
    wait_d(0)

    @pl.loop(0, n_full)
    def _(n):
        @pl.when(n == n_cut)
        def _():
            wait_d(1)

        with jax.named_scope("ph_fin_x"):
            x_pass(full(n), CHUNK, n).wait_recv()
        finish(full(n), CHUNK, n)

    x_pass(n_full * CHUNK, LANES, n_full).wait_recv()
    finish(n_full * CHUNK, tail, n_full)
    for k, p in enumerate(col_peers):
        remote(msg_d.at[p], got_d.at[c], d_sem.at[0, k], d_sem.at[1, k], r, p).wait_send()
    remote(part.at[r], half.at[0], xs_sem.at[0], xr_sem.at[0], r_s, c).wait_send()


def solution(mesh):
    n_row = mesh.shape["row"]
    n_col = mesh.shape["col"]
    amp_spec = P("row", "col")
    wide_spec = P(None, "col")

    def local_sweep(t_blk, d_blk, oovv_blk, vvvv_blk, oooo_full, wd_blk, wx_blk):
        rows_dev, cols_dev = t_blk.shape
        n_occ = math.isqrt(oooo_full.shape[0])
        n_virt = wd_blk.shape[0] // n_occ
        occ, vir = n_occ // n_row, n_virt // n_col
        n_pair = occ * occ
        n_chunk = cols_dev // CHUNK + 1
        wide = -(-cols_dev // LANES) * LANES
        kc, jb = wd_blk.shape
        perm = np.eye(rows_dev, dtype=BF16).reshape(occ, n_col, occ, rows_dev).transpose(1, 0, 2, 3).reshape(rows_dev, rows_dev)
        n_sq = n_occ * n_occ
        swap = np.eye(n_sq, dtype=BF16).reshape(n_occ, n_occ, n_sq).transpose(1, 0, 2).reshape(n_sq, n_sq)
        dma = pltpu.SemaphoreType.DMA
        vm = pltpu.VMEM
        hbm = pl.BlockSpec(memory_space=pl.ANY)
        block = (rows_dev, cols_dev)
        return pl.pallas_call(
            functools.partial(sweep_kernel, (n_occ, n_virt, n_row, n_col)),
            out_shape=pltpu.VMEM(block, F32),
            in_specs=[hbm] * 9,
            out_specs=pl.BlockSpec(memory_space=pltpu.VMEM),
            scratch_shapes=[
                vm(block, F32), vm((n_col,) + block, BF16), vm((n_row,) + block, BF16), vm((n_row,) + block, BF16),
                vm((kc, jb), BF16), vm((jb, kc), BF16), vm((jb, kc), BF16),
                vm((kc, n_virt), BF16), vm((n_virt, kc), BF16), vm((n_virt, jb), F32), vm((jb, n_virt), F32),
                vm((n_pair, n_virt, n_virt), F32), vm((n_pair, n_virt, n_virt), F32),
                vm((n_col, n_pair, wide), F32), vm((n_col, n_pair, wide), F32),
                vm((n_col, n_pair, wide), F32), vm((n_col, n_pair, wide), F32),
                vm((n_row, rows_dev, wide), F32), vm((2, rows_dev, wide), F32),
                vm((n_chunk, rows_dev, CHUNK), F32), vm((n_chunk, rows_dev, CHUNK), F32), vm((rows_dev, CHUNK), F32),
                vm((DEPTH, cols_dev, CHUNK), BF16), vm((cols_dev, cols_dev % CHUNK), BF16), vm(block, BF16), vm(oooo_full.shape, BF16),
                vm((rows_dev, rows_dev), BF16), vm((n_sq, n_sq), BF16),
                vm((rows_dev, n_sq), F32), vm((n_col, rows_dev, n_sq), F32),
                vm((n_row, rows_dev, rows_dev), BF16), vm((n_row, rows_dev, rows_dev), BF16),
                dma((9 + NQ,)), dma((DEPTH,)), dma((2,)), dma((3,)), dma((3, NQ)), dma((4,)), dma((2, NQ)), dma((2,)), dma((2, 4)),
                dma((2,)), dma((3,)), dma((3, cols_dev // WIDE + 1)), dma((3, 3)), dma((2,)), dma((2, RING)),
                dma((1,)), dma((n_chunk,)), dma((2, 3)), dma((2, 3)),
            ],
            compiler_params=pltpu.CompilerParams(
                collective_id=0, has_side_effects=True, vmem_limit_bytes=65536000),
        )(t_blk, d_blk, oovv_blk, vvvv_blk, oooo_full, wd_blk.T, wx_blk.T, jnp.asarray(perm), jnp.asarray(swap))

    return jax.shard_map(
        local_sweep, mesh=mesh,
        in_specs=(amp_spec, amp_spec, amp_spec, amp_spec, P(), wide_spec, wide_spec),
        out_specs=amp_spec, check_vma=False)
```

```python
import functools
import math

import jax
import jax.numpy as jnp
import numpy as np
from jax import lax
from jax.experimental import pallas as pl
from jax.experimental.pallas import tpu as pltpu
from jax.sharding import PartitionSpec as P

F32 = jnp.float32
BF16 = jnp.bfloat16
MESH = pl.DeviceIdType.MESH
CHUNK = 256
WIDE = 512
RING = 4
DEPTH = 4
LANES = 128
ROW_STEP, X_STEP, M_STEP = 3, 6, 14
D_FIRST, D_SECOND = 9, 13
P_FIRST, P_AHEAD = 2, 6
AHEAD = 2
OVER_Y = 1
NQ = 4


def sweep_kernel(
    dims,
    t_hbm, den_hbm, oovv_hbm, vvvv_hbm, oooo_hbm, wd_hbm, wx_hbm, perm_hbm, swap_hbm,
    out,
    t32, rows, lad, tcols, wd, wdt, wxt, tr, ta, r3, r5, sd, sp, msg_d, msg_p, got_d, got_p,
    part, half, xsend, xgot, turned, vbuf, vlast, oovv, oooo, perm, swap, xpart, xgot_part, m_mine, m_got,
    in_sem, vb_sem, loc_sem, ts_sem, tr_sem, ls_sem, lr_sem, ly_sem, g_sem,
    rx_sem, ps_sem, pr_sem, ds_sem, d_sem, hs_sem, hr_sem, xs_sem, xr_sem, x_sem, m_sem,
):
    n_occ, n_virt, n_row, n_col = dims
    rows_dev, cols_dev = t32.shape
    occ = n_occ // n_row
    vir = n_virt // n_col
    qrows = rows_dev // NQ
    n_full = cols_dev // CHUNK
    tail = cols_dev - n_full * CHUNK
    r = lax.axis_index("row")
    c = lax.axis_index("col")
    x, u = r // 2, r % 2
    z, y = c // 2, c % 2
    c_y, c_z, c_d = 2 * z + 1 - y, 2 * (1 - z) + y, 2 * (1 - z) + 1 - y
    r_p, r_s, r_o = 2 * x + 1 - u, 2 * (1 - x) + u, 2 * (1 - x) + 1 - u
    col_peers = (c_y, c_z, c_d)
    row_peers = (r_p, r_s, r_o)

    def remote(src, dst, ssem, rsem, row, col):
        return pltpu.make_async_remote_copy(
            src_ref=src, dst_ref=dst, send_sem=ssem, recv_sem=rsem,
            device_id={"row": row, "col": col}, device_id_type=MESH)

    def load(src, dst, k):
        return pltpu.make_async_copy(src, dst, in_sem.at[k])

    def ld_t(q):
        at = pl.ds(q * qrows, qrows)
        return load(t_hbm.at[at, :], t32.at[at, :], 9 + q)

    for q in range(NQ):
        ld_t(q).start()
    ld_wx = load(wx_hbm, wxt, 1)
    ld_wd = load(wd_hbm, wdt, 2)
    ld_oovv = load(oovv_hbm, oovv, 3)
    ld_oooo = load(oooo_hbm, oooo, 4)
    ld_perm = load(perm_hbm, perm, 5)
    ld_swap = load(swap_hbm, swap, 6)
    ld_den = load(den_hbm, t32, 7)

    def fetch(off, width, slot):
        return pltpu.make_async_copy(vvvv_hbm.at[:, pl.ds(off, width)], vbuf.at[slot], vb_sem.at[slot])

    barrier = pltpu.get_barrier_semaphore()
    for p in col_peers:
        pl.semaphore_signal(barrier, inc=1, device_id={"row": r, "col": p}, device_id_type=MESH)
    for p in row_peers:
        pl.semaphore_signal(barrier, inc=1, device_id={"row": p, "col": c}, device_id_type=MESH)
    pl.semaphore_wait(barrier, 6)

    def piece(ref, k, q):
        return ref.at[k, pl.ds(pl.multiple_of(q * qrows, qrows), qrows), :]

    def send_y(q):
        return remote(piece(rows, c, q), piece(rows, c, q), ts_sem.at[0], tr_sem.at[0, q], r, c_y)

    def send_z(q):
        return remote(piece(rows, c, q), piece(rows, c, q), ts_sem.at[1], tr_sem.at[1, q], r, c_z)

    def send_dz(q):
        return remote(piece(rows, c_y, q), piece(rows, c_y, q), ts_sem.at[2], tr_sem.at[2, q], r, c_z)

    def send_dy(q):
        return remote(piece(rows, c_z, q), piece(rows, c_z, q), ts_sem.at[2], tr_sem.at[2, q], r, c_y)

    blk_x = 2 * (1 - x) + y

    def send_lx(q):
        return remote(piece(rows, blk_x, q), piece(lad, r, q), ls_sem.at[0], lr_sem.at[u, q], blk_x, c)

    def recv_lx(w, q):
        k = 2 * (1 - x) + w
        return remote(piece(lad, k, q), piece(lad, k, q), ls_sem.at[0], lr_sem.at[w, q], blk_x, c)

    def send_ly(w, q):
        k = 2 * (1 - x) + w
        return remote(piece(lad, k, q), piece(lad, k, q), ls_sem.at[1 + w], ly_sem.at[w], r, c_y)

    def send_lo(q):
        k = 2 * (1 - x) + 1 - y
        return remote(piece(rows, k, q), piece(lad, r, q), ls_sem.at[3], ly_sem.at[u], k, c)

    def go_lo(q):
        send_lo(q).start()

    own_ladder = z == 1 - x
    direct = u == y

    for q in range(NQ):
        ld_t(q).wait()
        rows[c, pl.ds(q * qrows, qrows), :] = t32[pl.ds(q * qrows, qrows), :].astype(BF16)
        if q < AHEAD:
            send_y(q).start()
            send_z(q).start()

            @pl.when(own_ladder)
            def _():
                send_lx(q).start()

    for ld in (ld_wd, ld_wx, ld_swap, ld_perm, ld_oovv, ld_oooo):
        ld.start()
    ld_den.start()
    for s in range(DEPTH):
        fetch(s * CHUNK, CHUNK, s).start()

    ld_last = load(vvvv_hbm.at[:, pl.ds(n_full * CHUNK, tail)], vlast, 8)
    ld_last.start()

    def send_row(q):
        return remote(piece(rows, c, q), piece(tcols, r, q), rx_sem.at[0], rx_sem.at[1], r_s, c)

    row_p = remote(rows.at[c], tcols.at[r], g_sem.at[0, 0], g_sem.at[1, 0], r_p, c)
    row_o = remote(tcols.at[r_s], tcols.at[r_s], g_sem.at[0, 1], g_sem.at[1, 1], r_p, c)
    row_p.start()
    send_row(0).start()
    tcols[r] = rows[c]

    with jax.named_scope("ph_turn_w"):
        ld_wd.wait()

        @pl.loop(0, wd.shape[0] // LANES)
        def _(m):
            at = pl.ds(pl.multiple_of(m * LANES, LANES), LANES)
            for b in range(0, wd.shape[1], LANES):
                w = min(LANES, wd.shape[1] - b)
                wd[at, b:b + w] = wdt[b:b + w, at].astype(F32).T.astype(BF16)

    def forward_ladder(q):
        @pl.when(direct)
        def _():
            for w in range(2):
                recv_lx(w, q).wait_recv()
                send_ly(w, q).start()

    ld_swap.wait()
    ld_wx.wait()

    def spread(i):
        lines = pl.ds(pl.multiple_of(i * n_occ, n_occ), n_occ)
        for ab in range(n_virt // n_occ):
            stack = []
            for t in range(n_occ):
                a = ab * n_occ + t
                lo = (a % vir) * n_virt
                stack.append(rows[a // vir, lines, lo:lo + n_virt])
            lines_k = jnp.dot(swap[...], jnp.concatenate(stack, axis=0), preferred_element_type=F32).astype(BF16)
            for k in range(n_occ):
                line = lines_k[k * n_occ:(k + 1) * n_occ]
                tr[k * n_virt + ab * n_occ:k * n_virt + (ab + 1) * n_occ, :] = line
                ta[ab * n_occ:(ab + 1) * n_occ, k * n_virt:(k + 1) * n_virt] = line

    def particle_hole(i, between):
        with jax.named_scope("ph_spread"):
            spread(i)
        with jax.named_scope("ph_r5"):
            r5[...] = jnp.dot(wxt[...], tr[...], preferred_element_type=F32)
            r3[...] = jnp.dot(ta[...], wd[...], preferred_element_type=F32)
        between()
        with jax.named_scope("ph_diff"):
            for j in range(occ):
                diff = r3[:, j * n_virt:(j + 1) * n_virt] - r5[j * n_virt:(j + 1) * n_virt, :]
                sd[i * occ + j] = diff
                sp[j * occ + i] = diff.T

    lad_p = remote(rows.at[r_p], lad.at[r], g_sem.at[0, 3], g_sem.at[1, 3], r_p, c)

    def stage(q):
        send_z(q).wait_recv()

        @pl.when(jnp.logical_not(own_ladder))
        def _():
            send_lx(q).start()

        send_y(q).wait_recv()

        @pl.when(q == OVER_Y)
        def _():
            send_dy(q).start()

        @pl.when(q != OVER_Y)
        def _():
            send_dz(q).start()

        @pl.when(q + AHEAD < NQ)
        def _():
            send_y(q + AHEAD).start()
            send_z(q + AHEAD).start()

            @pl.when(own_ladder)
            def _():
                send_lx(q + AHEAD).start()

    def on_step(q, step, act, *args):
        @pl.when(q == step)
        def _():
            act(*args)

    def go_row(q):
        send_row(q).start()

    with jax.named_scope("ph_stages"):
        stage(0)
        stage(1)

    @pl.loop(0, NQ)
    def _(q):
        on_step(q, 2, forward_ladder, 2)
        send_dz(q).wait_recv()

        @pl.when(q == NQ - 1)
        def _():
            lad_p.start()

        on_step(q, 0, go_lo, 0)

        def between():
            @pl.when(q + 2 < NQ)
            def _():
                stage(q + 2)

            on_step(q, 0, forward_ladder, 1)
            on_step(q, 1, go_row, 1)
            on_step(q, 2, forward_ladder, 3)
            on_step(q, 2, go_row, 2)
            on_step(q, 3, go_row, 3)

        particle_hole(q, between)

    n_pair = occ * occ
    pad = pl.ds(cols_dev - tail, LANES)
    for k in range(n_col):
        msg_p[k, :, pad] = jnp.zeros((n_pair, LANES), F32)
        msg_d[k, :, pad] = jnp.zeros((n_pair, LANES), F32)
        part[k, :, pad] = jnp.zeros((rows_dev, LANES), F32)

    @pl.loop(0, n_col)
    def _(k):
        for a in range(vir):
            msg_p[k, :, a * n_virt:(a + 1) * n_virt] = sp[:, k * vir + a, :]

    def p_send(off, width, n, k, p):
        at = pl.ds(off, width)
        return remote(msg_p.at[p, :, at], got_p.at[c, :, at], ps_sem.at[0], pr_sem.at[k, n], r, p)

    n_wide = cols_dev // WIDE
    chunks = [(n * WIDE, WIDE) for n in range(n_wide)] + [(n_wide * WIDE, LANES)]
    def go_p(first, last):
        for n, (off, width) in enumerate(chunks[first:last], first):
            for k, p in enumerate(col_peers):
                p_send(off, width, n, k, p).start()

    go_p(0, P_FIRST)
    own_p = pltpu.make_async_copy(msg_p.at[c], got_p.at[c], loc_sem.at[0])
    own_p.start()

    d_cut = n_full // 2 * CHUNK
    d_halves = ((0, d_cut), (d_cut, msg_d.shape[2] - d_cut))

    def d_send(w, k, p):
        at = pl.ds(*d_halves[w])
        return remote(msg_d.at[p, :, at], got_d.at[c, :, at], ds_sem.at[0], d_sem.at[w, k], r, p)

    own_d = pltpu.make_async_copy(msg_d.at[c], got_d.at[c], loc_sem.at[1])

    def go_d(w):
        for k, p in enumerate(col_peers):
            d_send(w, k, p).start()

    def form_d():
        @pl.loop(0, n_col)
        def _(k):
            for a in range(vir):
                msg_d[k, :, a * n_virt:(a + 1) * n_virt] = sd[:, k * vir + a, :]

        go_d(0)
        own_d.start()

    ld_perm.wait()

    def permute(k, src):
        for off in range(0, cols_dev, 4 * LANES):
            width = min(4 * LANES, cols_dev - off)
            block = jnp.dot(perm[...], src[:, off:off + width], preferred_element_type=F32)
            lad[k, :, off:off + width] = block.astype(BF16)

    permute(r, rows.at[r])
    lad_p.wait_recv()
    permute(r_p, lad.at[r_p])

    @pl.when(jnp.logical_not(direct))
    def _():
        for w in range(2):
            whole = lad.at[2 * (1 - x) + w]
            remote(whole, whole, ls_sem.at[1 + w], ly_sem.at[w], r, c_y).wait_recv()

    @pl.when(direct)
    def _():
        for w in range(2):
            recv_lx(w, 0).wait_recv()
        for w in range(2):
            rest = lad.at[2 * (1 - x) + w, pl.ds(qrows, rows_dev - qrows), :]
            remote(rest, rest, ls_sem.at[1 + w], ly_sem.at[w], r, c_y).wait_send()

    go_p(P_FIRST, P_AHEAD)

    @pl.loop(0, 2)
    def _(w):
        permute(2 * (1 - x) + w, lad.at[2 * (1 - x) + w])

    own_p.wait()


    def h_send(off, width, n, w):
        at = pl.ds(off, width)
        return remote(part.at[2 * w + 1 - u, :, at], half.at[w, :, at], hs_sem.at[w], hr_sem.at[w, n % RING], r_p, c)

    def x_pass(off, width, n):
        return remote(xsend.at[n, :, pl.ds(0, width)], xgot.at[n, :, pl.ds(0, width)], xs_sem.at[0], xr_sem.at[n], r_s, c)

    def across(off, width, n):
        at = pl.ds(off, width)
        with jax.named_scope("ph_wait_h"):
            for w in range(2):
                h_send(off, width, n, w).wait_recv()
        xsend[n, :, 0:width] = part[2 * (1 - x) + u, :, at] + half[1 - x, :, at]
        x_pass(off, width, n).start()

    def ladder(off, width, n, v_ref, arrive):
        at = pl.ds(off, width)
        with jax.named_scope("ph_dot"):
            t_all = lad[...].reshape(n_row * rows_dev, cols_dev)
            prod = jnp.dot(t_all, v_ref[...], preferred_element_type=F32)
            part[:, :, pl.ds(off, prod.shape[1])] = prod.reshape(n_row, rows_dev, prod.shape[1])
        arrive()
        mine = pl.ds(pl.multiple_of(r * n_pair, n_pair), n_pair)
        for k in range(n_col):
            part[k, mine, at] += got_p[k, :, at]
        for w in range(2):
            h_send(off, width, n, w).start()

    def x_send(k, p):
        return remote(xpart, xgot_part.at[c], x_sem.at[0], x_sem.at[1 + k], r, p)

    def form_x():
        row_p.wait_recv()
        row_o.wait_recv()
        ld_oovv.wait()
        for k in range(n_row):
            xpart[:, k * rows_dev:(k + 1) * rows_dev] = lax.dot_general(
                oovv[...], tcols[k], (((1,), (1,)), ((), ())), preferred_element_type=F32)
        for k, p in enumerate(col_peers):
            x_send(k, p).start()

    def m_send(k, p):
        return remote(m_mine.at[p], m_got.at[r], m_sem.at[0], m_sem.at[1 + k], p, c)

    def form_m():
        for k, p in enumerate(col_peers):
            x_send(k, p).wait_recv()
        xgot_part[c] = xpart[...]
        x_sum = xgot_part[0] + xgot_part[1] + xgot_part[2] + xgot_part[3]
        ld_oooo.wait()
        hole = (oooo[pl.ds(pl.multiple_of(r * rows_dev, rows_dev), rows_dev), :].astype(F32) + 0.5 * x_sum)
        for k in range(n_row):
            m_mine[k] = hole[:, k * rows_dev:(k + 1) * rows_dev].astype(BF16)
        for k, p in enumerate(row_peers):
            m_send(k, p).start()
        m_got[r] = m_mine[r]

    per = WIDE // CHUNK

    @pl.loop(0, n_full)
    def _(n):
        off = pl.multiple_of(n * CHUNK, CHUNK)
        with jax.named_scope("ph_wait_v"):
            fetch(off, CHUNK, n % DEPTH).wait()
        m = n // per
        p_off = pl.multiple_of(m * WIDE, WIDE)

        def arrive():
            @pl.when(n % per == 0)
            def _():
                for k, p in enumerate(col_peers):
                    p_send(p_off, WIDE, m, k, p).wait_recv()

        ladder(off, CHUNK, n, vbuf.at[n % DEPTH], arrive)

        @pl.when(n + DEPTH < n_full)
        def _():
            fetch(pl.multiple_of((n + DEPTH) * CHUNK, CHUNK), CHUNK, n % DEPTH).start()

        @pl.when(jnp.logical_and(n % per == 0, m + P_AHEAD < n_wide))
        def _():
            later = pl.multiple_of((m + P_AHEAD) * WIDE, WIDE)
            for k, p in enumerate(col_peers):
                p_send(later, WIDE, m + P_AHEAD, k, p).start()

        @pl.when(n == (n_wide - P_AHEAD) * per)
        def _():
            for k, p in enumerate(col_peers):
                p_send(n_wide * WIDE, LANES, n_wide, k, p).start()

        @pl.when(n == ROW_STEP)
        def _():
            remote(tcols.at[r_s], tcols.at[r_s], rx_sem.at[0], rx_sem.at[1], r_s, c).wait_recv()
            row_o.start()

        @pl.when(n == X_STEP)
        def _():
            with jax.named_scope("ph_form_x"):
                form_x()

        @pl.when(n == M_STEP)
        def _():
            with jax.named_scope("ph_form_m"):
                form_m()

        @pl.when(n == D_FIRST)
        def _():
            with jax.named_scope("ph_form_d"):
                form_d()

        @pl.when(n == D_SECOND)
        def _():
            go_d(1)

        @pl.when(n == 0)
        def _():
            across(0, CHUNK, 0)

        @pl.when(n >= 2)
        def _():
            across(pl.multiple_of((n - 1) * CHUNK, CHUNK), CHUNK, n - 1)

    ld_last.wait()
    def arrive_last():
        for k, p in enumerate(col_peers):
            p_send(n_wide * WIDE, LANES, n_wide, k, p).wait_recv()

    ladder(n_full * CHUNK, LANES, n_full, vlast, arrive_last)
    across((n_full - 1) * CHUNK, CHUNK, n_full - 1)
    across(n_full * CHUNK, LANES, n_full)

    with jax.named_scope("ph_fin_m"):
        for k, p in enumerate(row_peers):
            m_send(k, p).wait_recv()
    ld_den.wait()

    def hole_term(off, width):
        at = pl.ds(off, width)
        total = None
        for k in range(n_row):
            term = lax.dot_general(
                m_got[k], tcols[k, :, at], (((0,), (0,)), ((), ())), preferred_element_type=F32)
            total = term if total is None else total + term
        part[r_s, :, at] = total + oovv[:, at].astype(F32)
        part[r, :, pl.ds(off, width)] += half[x, :, at]

    def finish(off, width, n):
        at = pl.ds(off, width)
        own = part[r, :, at] + xgot[n, :, 0:width]
        for jh in range(n_col):
            v = own[jh * n_pair:(jh + 1) * n_pair] + got_d[jh, :, at]
            for i in range(occ):
                lo = i * n_occ + jh * occ
                turned[lo:lo + occ, 0:width] = v[i * occ:(i + 1) * occ]
        out[:, at] = (part[r_s, :, at] + turned[:, 0:width]) / t32[:, at]

    def full(n):
        return pl.multiple_of(n * CHUNK, CHUNK)

    @pl.loop(0, n_full)
    def _(n):
        hole_term(full(n), CHUNK)

    hole_term(n_full * CHUNK, tail)
    n_cut = d_cut // CHUNK

    def wait_d(w):
        with jax.named_scope("ph_fin_d"):
            for k, p in enumerate(col_peers):
                d_send(w, k, p).wait_recv()

    lad_p.wait_send()
    send_lo(0).wait_send()
    row_p.wait_send()
    row_o.wait_send()
    own = rows.at[c]
    for k in range(3):
        remote(own, own, ts_sem.at[k], tr_sem.at[0, 0], r, c_y).wait_send()
    remote(own, own, ls_sem.at[0], tr_sem.at[0, 0], r, c_y).wait_send()
    remote(own, own, rx_sem.at[0], rx_sem.at[1], r_s, c).wait_send()
    three = pl.ds(0, 3)
    remote(m_mine.at[three], m_got.at[three], m_sem.at[0], m_sem.at[1], r_p, c).wait_send()
    remote(xgot_part.at[three], xgot_part.at[three], x_sem.at[0], x_sem.at[1], r, c_y).wait_send()
    remote(msg_p.at[three], got_p.at[three], ps_sem.at[0], pr_sem.at[0, 0], r, c_y).wait_send()
    for w in range(2):
        remote(part.at[2 * w + 1 - u], half.at[w], hs_sem.at[w], hr_sem.at[w, 0], r_p, c).wait_send()

    own_d.wait()
    wait_d(0)

    @pl.loop(0, n_full)
    def _(n):
        @pl.when(n == n_cut)
        def _():
            wait_d(1)

        with jax.named_scope("ph_fin_x"):
            x_pass(full(n), CHUNK, n).wait_recv()
        finish(full(n), CHUNK, n)

    x_pass(n_full * CHUNK, LANES, n_full).wait_recv()
    finish(n_full * CHUNK, tail, n_full)
    remote(msg_d.at[three], got_d.at[three], ds_sem.at[0], d_sem.at[0, 0], r, c_y).wait_send()
    remote(part.at[r], half.at[0], xs_sem.at[0], xr_sem.at[0], r_s, c).wait_send()


def solution(mesh):
    n_row = mesh.shape["row"]
    n_col = mesh.shape["col"]
    amp_spec = P("row", "col")
    wide_spec = P(None, "col")

    def local_sweep(t_blk, d_blk, oovv_blk, vvvv_blk, oooo_full, wd_blk, wx_blk):
        rows_dev, cols_dev = t_blk.shape
        n_occ = math.isqrt(oooo_full.shape[0])
        n_virt = wd_blk.shape[0] // n_occ
        occ, vir = n_occ // n_row, n_virt // n_col
        n_pair = occ * occ
        n_chunk = cols_dev // CHUNK + 1
        wide = -(-cols_dev // LANES) * LANES
        kc, jb = wd_blk.shape
        perm = np.eye(rows_dev, dtype=BF16).reshape(occ, n_col, occ, rows_dev).transpose(1, 0, 2, 3).reshape(rows_dev, rows_dev)
        n_sq = n_occ * n_occ
        swap = np.eye(n_sq, dtype=BF16).reshape(n_occ, n_occ, n_sq).transpose(1, 0, 2).reshape(n_sq, n_sq)
        dma = pltpu.SemaphoreType.DMA
        vm = pltpu.VMEM
        hbm = pl.BlockSpec(memory_space=pl.ANY)
        block = (rows_dev, cols_dev)
        return pl.pallas_call(
            functools.partial(sweep_kernel, (n_occ, n_virt, n_row, n_col)),
            out_shape=pltpu.VMEM(block, F32),
            in_specs=[hbm] * 9,
            out_specs=pl.BlockSpec(memory_space=pltpu.VMEM),
            scratch_shapes=[
                vm(block, F32), vm((n_col,) + block, BF16), vm((n_row,) + block, BF16), vm((n_row,) + block, BF16),
                vm((kc, jb), BF16), vm((jb, kc), BF16), vm((jb, kc), BF16),
                vm((kc, n_virt), BF16), vm((n_virt, kc), BF16), vm((n_virt, jb), F32), vm((jb, n_virt), F32),
                vm((n_pair, n_virt, n_virt), F32), vm((n_pair, n_virt, n_virt), F32),
                vm((n_col, n_pair, wide), F32), vm((n_col, n_pair, wide), F32),
                vm((n_col, n_pair, wide), F32), vm((n_col, n_pair, wide), F32),
                vm((n_row, rows_dev, wide), F32), vm((2, rows_dev, wide), F32),
                vm((n_chunk, rows_dev, CHUNK), F32), vm((n_chunk, rows_dev, CHUNK), F32), vm((rows_dev, CHUNK), F32),
                vm((DEPTH, cols_dev, CHUNK), BF16), vm((cols_dev, cols_dev % CHUNK), BF16), vm(block, BF16), vm(oooo_full.shape, BF16),
                vm((rows_dev, rows_dev), BF16), vm((n_sq, n_sq), BF16),
                vm((rows_dev, n_sq), F32), vm((n_col, rows_dev, n_sq), F32),
                vm((n_row, rows_dev, rows_dev), BF16), vm((n_row, rows_dev, rows_dev), BF16),
                dma((9 + NQ,)), dma((DEPTH,)), dma((2,)), dma((3,)), dma((3, NQ)), dma((4,)), dma((2, NQ)), dma((2,)), dma((2, 4)),
                dma((2,)), dma((1,)), dma((3, cols_dev // WIDE + 1)), dma((1,)), dma((2, 3)), dma((2,)), dma((2, RING)),
                dma((1,)), dma((n_chunk,)), dma((4,)), dma((4,)),
            ],
            compiler_params=pltpu.CompilerParams(
                collective_id=0, has_side_effects=True, vmem_limit_bytes=65536000),
        )(t_blk, d_blk, oovv_blk, vvvv_blk, oooo_full, wd_blk.T, wx_blk.T, jnp.asarray(perm), jnp.asarray(swap))

    return jax.shard_map(
        local_sweep, mesh=mesh,
        in_specs=(amp_spec, amp_spec, amp_spec, amp_spec, P(), wide_spec, wide_spec),
        out_specs=amp_spec, check_vma=False)
```
